32 devices in a mesh: dp: 8 (over y, x, core), mp: 4 (over z).
Axes of the slice: x: 2, y: 2, z: 4, core: 2. Of those that a mesh axis runs over, the one named last changes fastest.
Arguments:
- tokens: bfloat16 [6144, 6144], P('dp', 'mp'), may hold values from -6 to 6
- ln_gain: bfloat16 [6144], P('mp'), may hold values from 0.5 to 1.5
- weights: bfloat16 [6144, 12288], P('dp', 'mp'), may hold values from -0.078125 to 0.078125
- grad_partials: bfloat16 [8, 6144, 12288], P('dp', None, 'mp'), may hold values from -40 to 40, as said below
Outputs:
- hidden: bfloat16 [6144, 12288], P('dp', 'mp')
- perturbed_weights: bfloat16 [6144, 12288], P('dp', 'mp')
The draws below stay inside these ranges and needn't reach their ends.
Inputs may be any that keep to these rules, and one draw needn't show every extreme that they name: `grad_partials`: each slice along the first dimension is one data shard's gradient.
All inputs are finite; a program needn't handle non-finite values.
Results may differ from the reference program's by a relative error of at most 0.012.
Values may be sent and summed in bfloat16 or wider, within the bound.
A program may use at most 192 MiB of HBM per device.

```python
import math
import jax
import jax.numpy as jnp
from jax import lax

D = 6144
FF = 12288
TOKENS = 6144
N_DP = 8
N_MP = 4


def draw_grad_partials(key, part):
    key_rows, key_cols, key_own = jax.random.split(key, 3)
    row_scale = jnp.exp(jax.random.uniform(key_rows, (1, D, 1), jnp.float32, 0.0, math.log(10.0)))
    col_scale = jnp.exp(jax.random.uniform(key_cols, (1, 1, FF), jnp.float32, 0.0, math.log(10.0)))
    ramp = (3.0 ** (jnp.arange(N_DP, dtype=jnp.float32) / max(N_DP - 1, 1))).reshape(N_DP, 1, 1)
    row_place = (jnp.arange(D, dtype=jnp.float32) / D).reshape(1, D, 1)
    block_width = FF // N_MP
    col_place = ((jnp.arange(FF) % block_width).astype(jnp.float32) / block_width).reshape(1, 1, FF)
    rise = 3.0
    own = jnp.clip(jax.random.normal(key_own, (N_DP, D, FF), jnp.float32), -6.0, 6.0)
    values = ramp * row_scale * col_scale * own
    position = rise ** (row_place - 1.0) * rise ** (col_place - 1.0)
    return (0.01 * values * position).astype(jnp.bfloat16)


def block_scale(stream_key, dims, cuts, smallest, largest):
    gain, own = 1.0, jax.random.fold_in(stream_key, 6)
    for axis_at, parts in cuts:
        draws = jnp.exp(jax.random.uniform(jax.random.fold_in(own, axis_at), (parts,), jnp.float32, smallest / len(cuts), largest / len(cuts)))
        gain = gain * jnp.repeat(draws, dims[axis_at] // parts).reshape([-1 if axis == axis_at else 1 for axis in range(len(dims))])
    return gain


def noise(stream_key, extent, scale, limit, shards=(), held_as=jnp.bfloat16):
    factor_of = block_scale(stream_key, extent, shards, -0.22, 0.18) if shards else 1.0
    drawn = jax.random.normal(stream_key, extent, jnp.float32) * scale * factor_of
    return jnp.minimum(jnp.maximum(drawn, -limit), limit).astype(held_as)


def setup_inputs(seed: int = 0) -> dict:
    arg_keys = jax.random.split(jax.random.key(seed), 5)
    return {
        "tokens": noise(arg_keys[0], (TOKENS, D), 1.0, 6.0, ((0, 8), (1, 4))),
        "ln_gain": jnp.clip(1.0 + 0.1 * jax.random.normal(arg_keys[1], (D,), jnp.float32), 0.5, 1.5).astype(jnp.bfloat16),
        "weights": noise(arg_keys[2], (D, FF), D ** -0.5, 0.078125, ((0, 8), (1, 4))),
        "grad_partials": draw_grad_partials(jax.random.fold_in(arg_keys[4], 71), 0),
    }


def reference(tokens, ln_gain, weights, grad_partials):

    def add_shard(index, total):
        return total + grad_partials[index].astype(jnp.float32)
    grad = lax.fori_loop(0, N_DP, add_shard, jnp.zeros((D, FF), jnp.float32))
    squares = jnp.sum(grad * grad)
    scale = 0.7 * math.sqrt(FF) / jnp.sqrt(squares + 1e-12)
    perturbed = (weights.astype(jnp.float32) + scale * grad).astype(jnp.bfloat16)
    values = tokens.astype(jnp.float32)
    center = lax.optimization_barrier(jnp.mean(values, axis=1, keepdims=True))
    spread = lax.optimization_barrier(jnp.mean((values - center) ** 2, axis=1, keepdims=True))
    normed = ((values - center) / jnp.sqrt(spread + 1e-06) * ln_gain.astype(jnp.float32)).astype(jnp.bfloat16)
    pre = jnp.dot(normed, perturbed, preferred_element_type=jnp.float32)
    hidden = jax.nn.gelu(pre, approximate=False).astype(jnp.bfloat16)
    return (hidden, perturbed)
```

```python
import functools
import math

import jax
import jax.numpy as jnp
from jax import lax
from jax.experimental import pallas as pl
from jax.experimental.pallas import tpu as pltpu
from jax.sharding import PartitionSpec as P

SUBS = 6
AHEAD = 2
CHUNK = 128
GROUP = 3
VMEM_LIMIT = 66 * 1000 * 1000


def power_of_two(n):
    return n & (n - 1) == 0


def chip_at(pos, n):
    if not power_of_two(n):
        return pos
    bits = n.bit_length() - 1
    out = 0
    for b in range(bits):
        out = out + ((pos // 2**b + pos // 2 ** (b + 1)) % 2) * 2**b
    return out


def position_of(chip, n):
    if not power_of_two(n):
        return chip
    bits = n.bit_length() - 1
    above, out = 0, 0
    for b in reversed(range(bits)):
        above = (chip // 2**b + above) % 2
        out = out + above * 2**b
    return out


def ring(n):
    me = lax.axis_index("dp")
    chip, core = me // 2, me % 2
    pos = position_of(chip, n)
    right = chip_at((pos + 1) % n, n) * 2 + core
    left = chip_at((pos + n - 1) % n, n) * 2 + core
    return pos, core, (right, left), chip * 2 + 1 - core


def greet(peers, meanwhile=None):
    barrier = pltpu.get_barrier_semaphore()
    for axis, peer in peers:
        pl.semaphore_signal(
            barrier, inc=1, device_id={axis: peer}, device_id_type=pl.DeviceIdType.MESH
        )
    if meanwhile is not None:
        meanwhile()
    pl.semaphore_wait(barrier, len(peers))


def others(axis, size):
    me = lax.axis_index(axis)
    return [(axis, (me + k) % size) for k in range(1, size)]


def remote(src, dst, send, recv, peer, axis="dp"):
    return pltpu.make_async_remote_copy(
        src_ref=src,
        dst_ref=dst,
        send_sem=send,
        recv_sem=recv,
        device_id={axis: peer},
        device_id_type=pl.DeviceIdType.MESH,
    )


def scatter_kernel(
    n, n_mp, radius, g_ref, w_ref, gain_ref, out_ref, gains_ref,
    part, recv, own, grad, sq_ref, stat, sums, gains,
    part_send, part_recv, hop_send, hop_recv, own_sem,
    stat_send, stat_recv, sums_send, sums_recv, gain_send, gain_recv,
):
    pos, core, hops, partner = ring(n)
    rows, half = part.shape[2], part.shape[3]
    sub = rows // SUBS
    total = n * SUBS
    tile = 16
    dp_peers, mp_peers = others("dp", 2 * n), others("mp", n_mp)
    greet(dp_peers + mp_peers)

    def block(t, d, which):
        s, i = t // SUBS, t % SUBS
        target = (pos + n - 1 - s + n) % n if d == 0 else (pos + 1 + s) % n
        start = (chip_at(target, n) * 2 + which) * rows + i * sub
        return g_ref.at[pl.ds(pl.multiple_of(start, tile), sub), pl.ds(d * half, half)]

    def piece(ref, t, d):
        return ref.at[t // SUBS, d, pl.ds(pl.multiple_of((t % SUBS) * sub, tile), sub)]

    def push(t, d):
        at = t * 2 + d
        return remote(
            block(t, d, 1 - core), piece(part, t, d), part_send.at[at], part_recv.at[at], partner
        )

    def load(t, d):
        return pltpu.make_async_copy(block(t, d, core), own.at[t % 2, d], own_sem.at[(t % 2) * 2 + d])

    def hop(t, d, src):
        at = t * 2 + d
        return remote(piece(src, t, d), piece(recv, t, d), hop_send.at[at], hop_recv.at[at], hops[d])

    for d in range(2):
        load(0, d).start()

    @pl.loop(0, SUBS)
    def _(t):
        for d in range(2):
            push(t, d).start()

    place = lax.axis_index("mp")
    fetch = pltpu.make_async_copy(w_ref, out_ref, own_sem.at[4])
    fetch.start()
    gain_copies = [
        remote(gain_ref, gains.at[place], gain_send.at[k], gain_recv.at[k], peer, axis)
        for k, (axis, peer) in enumerate(mp_peers)
    ]
    for copy in gain_copies:
        copy.start()
    gains[place] = gain_ref[...]
    sq_ref[...] = jnp.zeros_like(sq_ref)

    def step(t, first, last):
        @pl.when(t + 1 < total)
        def _():
            for d in range(2):
                load(t + 1, d).start()

        @pl.when(t + SUBS < total)
        def _():
            for d in range(2):
                push(t + SUBS, d).start()

        for d in range(2):
            load(t, d).wait()
            push(t, d).wait_recv()
            if not first:
                hop(t - SUBS, d, recv).wait_recv()
            source = piece(part, t, d)
            came = None if first else piece(recv, t - SUBS, d)
            mine = own.at[t % 2, d]

            @pl.loop(0, sub // tile)
            def _(r):
                at = pl.ds(pl.multiple_of(r * tile, tile), tile)
                value = mine[at, :].astype(jnp.float32) + source[at, :].astype(jnp.float32)
                if not first:
                    value = value + came[at, :].astype(jnp.float32)
                if last:
                    row = pl.multiple_of((t % SUBS) * sub + r * tile, tile)
                    grad[pl.ds(row, tile), d * half : (d + 1) * half] = value
                    squared = value * value
                    sq_ref[...] += squared[:8] + squared[8:]
                elif first:
                    source[at, :] = value.astype(jnp.bfloat16)
                else:
                    came[at, :] = value.astype(jnp.bfloat16)

        if not last:
            for d in range(2):
                at = t * 2 + d
                src = piece(part, t, d) if first else piece(recv, t - SUBS, d)
                remote(src, piece(recv, t, d), hop_send.at[at], hop_recv.at[at], hops[d]).start()

    @pl.loop(0, SUBS)
    def _(t):
        step(t, True, False)

    @pl.loop(SUBS, total - SUBS)
    def _(t):
        step(t, False, False)

    @pl.loop(total - SUBS, total)
    def _(t):
        step(t, False, True)

    folded = sq_ref[:, :128]
    for c in range(1, half // 128):
        folded = folded + sq_ref[:, c * 128 : (c + 1) * 128]
    stat[0] = folded

    @pl.loop(0, total)
    def _(t):
        for d in range(2):
            push(t, d).wait_send()

    @pl.loop(0, total - SUBS)
    def _(t):
        for d in range(2):
            hop(t, d, recv).wait_send()

    def share(slots, peers, send, arrive):
        copies = [
            remote(slots.at[0], slots.at[k + 1], send.at[k], arrive.at[k], peer, axis)
            for k, (axis, peer) in enumerate(peers)
        ]
        for copy in copies:
            copy.start()
        for copy in copies:
            copy.wait()
        return jnp.sum(slots[...], axis=0)

    sums[0] = share(stat, dp_peers, stat_send, stat_recv)
    for copy in gain_copies:
        copy.wait()
    gains_ref[...] = gains[...]
    fetch.wait()
    every = share(sums, mp_peers, sums_send, sums_recv)
    squares = jnp.sum(jnp.sum(every, axis=0, keepdims=True), axis=1, keepdims=True)
    scale = radius / jnp.sqrt(squares + 1e-12)

    @pl.loop(0, rows // tile)
    def _(r):
        at = pl.ds(pl.multiple_of(r * tile, tile), tile)
        value = out_ref[at, :].astype(jnp.float32) + scale * grad[at, :]
        out_ref[at, :] = value.astype(jnp.bfloat16)


def reduce_rows(n, n_mp, radius, grads, weights, gain):
    depth, cols = grads.shape
    rows, half = depth // (2 * n), cols // 2
    sub = rows // SUBS
    dma = pltpu.SemaphoreType.DMA
    return pl.pallas_call(
        functools.partial(scatter_kernel, n, n_mp, radius),
        out_shape=(
            jax.ShapeDtypeStruct((rows, cols), jnp.bfloat16),
            jax.ShapeDtypeStruct((n_mp, *gain.shape), jnp.float32),
        ),
        in_specs=[
            pl.BlockSpec(memory_space=pl.ANY),
            pl.BlockSpec(memory_space=pl.ANY),
            pl.BlockSpec(memory_space=pltpu.VMEM),
        ],
        out_specs=(
            pl.BlockSpec(memory_space=pltpu.VMEM),
            pl.BlockSpec(memory_space=pltpu.VMEM),
        ),
        scratch_shapes=[
            pltpu.VMEM((n, 2, rows, half), jnp.bfloat16),
            pltpu.VMEM((n - 1, 2, rows, half), jnp.bfloat16),
            pltpu.VMEM((2, 2, sub, half), jnp.bfloat16),
            pltpu.VMEM((rows, cols), jnp.float32),
            pltpu.VMEM((8, half), jnp.float32),
            pltpu.VMEM((2 * n, 8, 128), jnp.float32),
            pltpu.VMEM((n_mp, 8, 128), jnp.float32),
            pltpu.VMEM((n_mp, *gain.shape), jnp.float32),
            dma((n * SUBS * 2,)),
            dma((n * SUBS * 2,)),
            dma(((n - 1) * SUBS * 2,)),
            dma(((n - 1) * SUBS * 2,)),
            dma((5,)),
            dma((2 * n - 1,)),
            dma((2 * n - 1,)),
            dma((n_mp - 1,)),
            dma((n_mp - 1,)),
            dma((n_mp - 1,)),
            dma((n_mp - 1,)),
        ],
        compiler_params=pltpu.CompilerParams(
            collective_id=1, has_side_effects=True, vmem_limit_bytes=VMEM_LIMIT
        ),
        cost_estimate=pl.CostEstimate(
            flops=200 * 10**9, bytes_accessed=3 * grads.size, transcendentals=0
        ),
        name="reduce_rows",
    )(grads, weights, gain)


def gather_kernel(
    n, x_ref, gain_ref, p_ref, out_ref, normed, buf, pre_ref,
    hop_send, hop_recv, part_send, part_recv, own_sem, x_sem,
):
    pos, core, hops, partner = ring(n)
    rows, width = buf.shape[3] // 2, buf.shape[4]
    half = SUBS * width
    greet([("dp", peer) for peer in (*hops, partner)])

    def mine(i, d):
        return p_ref.at[:, pl.ds(pl.multiple_of(d * half + i * width, 128), width)]

    def piece(s, i, d, which):
        return buf.at[s, d, i, pl.ds(pl.multiple_of(which * rows, 16), rows)]

    def hop(s, i, d, src):
        at = ((s - 1) * SUBS + i) * 2 + d
        return remote(src, piece(s, i, d, core), hop_send.at[at], hop_recv.at[at], hops[d])

    def push(s, i, d, src):
        at = (s * SUBS + i) * 2 + d
        return remote(src, piece(s, i, d, core), part_send.at[at], part_recv.at[at], partner)

    def pushed(s, i, d):
        at = (s * SUBS + i) * 2 + d
        there = piece(s, i, d, 1 - core)
        return remote(there, there, part_send.at[at], part_recv.at[at], partner)

    def keep(i, d):
        return pltpu.make_async_copy(mine(i, d), piece(0, i, d, core), own_sem.at[i * 2 + d])

    fetch = pltpu.make_async_copy(x_ref, normed, x_sem.at[0])
    fetch.start()
    for i in range(AHEAD):
        for d in range(2):
            hop(1, i, d, mine(i, d)).start()

    @pl.loop(0, SUBS)
    def _(i):
        for d in range(2):
            keep(i, d).start()
            push(0, i, d, mine(i, d)).start()

    pre_ref[...] = jnp.zeros_like(pre_ref)
    fetch.wait()

    @pl.loop(0, normed.shape[0] // 16)
    def _(r):
        at = pl.ds(pl.multiple_of(r * 16, 16), 16)
        values = normed[at, :].astype(jnp.float32)
        center = jnp.mean(values, axis=1, keepdims=True)
        moved = values - center
        spread = jnp.mean(moved * moved, axis=1, keepdims=True)
        scaled = moved * (1.0 / jnp.sqrt(spread + 1e-06)) * gain_ref[...]
        normed[at, :] = scaled.astype(jnp.bfloat16)

    def multiply(s, i):
        for d in range(2):
            pushed(s, i, d).wait_recv()
            owner = (pos + n - s) % n if d == 0 else (pos + s) % n
            cols = pl.ds(pl.multiple_of(chip_at(owner, n) * 2 * rows, 128), 2 * rows)
            out = pl.ds(pl.multiple_of(d * half + i * width, 128), width)
            pre_ref[:, out] += jnp.dot(
                normed[:, cols], buf[s, d, i], preferred_element_type=jnp.float32
            )

    def activate(i):
        tall = 64
        for d in range(2):
            cols = pl.ds(pl.multiple_of(d * half + i * width, 128), width)

            @pl.loop(0, pre_ref.shape[0] // tall)
            def _(r):
                at = pl.ds(pl.multiple_of(r * tall, tall), tall)
                pre = pre_ref[at, cols]
                value = 0.5 * pre * (1.0 + lax.erf(pre * math.sqrt(0.5)))
                out_ref[at, cols] = value.astype(jnp.bfloat16)

    @pl.loop(0, SUBS + n - 1)
    def _(wave):
        @pl.when(wave + AHEAD < SUBS)
        def _():
            for d in range(2):
                hop(1, wave + AHEAD, d, mine(wave + AHEAD, d)).start()

        for s in range(1, n):
            i = wave - (s - 1)

            @pl.when((i >= 0) & (i < SUBS))
            def _():
                for d in range(2):
                    hop(s, i, d, piece(s, i, d, core)).wait_recv()
                    if s < n - 1:
                        hop(s + 1, i, d, piece(s, i, d, core)).start()
                    push(s, i, d, piece(s, i, d, core)).start()

            if s == 1:

                @pl.when(wave < SUBS)
                def _():
                    for d in range(2):
                        keep(wave, d).wait()
                    multiply(0, wave)

            @pl.when((i >= 1) & (i <= SUBS))
            def _():
                multiply(s, i - 1)
                if s == n - 1:
                    activate(i - 1)

    @pl.loop(0, SUBS)
    def _(i):
        for d in range(2):
            for s in range(n):
                push(s, i, d, piece(s, i, d, core)).wait_send()
            for s in range(1, n):
                hop(s, i, d, piece(s, i, d, core)).wait_send()


def gather_matmul(n, feats, gains, perturbed):
    tokens, depth = feats.shape
    rows, cols = perturbed.shape
    half = cols // 2
    dma = pltpu.SemaphoreType.DMA
    return pl.pallas_call(
        functools.partial(gather_kernel, n),
        out_shape=jax.ShapeDtypeStruct((tokens, cols), jnp.bfloat16),
        in_specs=[
            pl.BlockSpec(memory_space=pl.ANY),
            pl.BlockSpec(memory_space=pltpu.VMEM),
            pl.BlockSpec(memory_space=pl.ANY),
        ],
        out_specs=pl.BlockSpec(memory_space=pltpu.VMEM),
        scratch_shapes=[
            pltpu.VMEM((tokens, depth), jnp.bfloat16),
            pltpu.VMEM((n, 2, SUBS, 2 * rows, half // SUBS), jnp.bfloat16),
            pltpu.VMEM((tokens, cols), jnp.float32),
            dma(((n - 1) * SUBS * 2,)),
            dma(((n - 1) * SUBS * 2,)),
            dma((n * SUBS * 2,)),
            dma((n * SUBS * 2,)),
            dma((SUBS * 2,)),
            dma((1,)),
        ],
        compiler_params=pltpu.CompilerParams(
            collective_id=2, has_side_effects=True, vmem_limit_bytes=VMEM_LIMIT
        ),
        cost_estimate=pl.CostEstimate(
            flops=2 * tokens * depth * cols,
            bytes_accessed=2 * depth * cols,
            transcendentals=0,
        ),
        name="gather_matmul",
    )(feats, gains, perturbed)


def ring_program(n, n_mp, radius, tokens, ln_gain, weights, grad_partials):
    feats = lax.all_gather(tokens, "mp", axis=1, tiled=True)
    gain = jnp.broadcast_to(ln_gain.astype(jnp.float32), (8, ln_gain.shape[0]))
    perturbed, gains = reduce_rows(n, n_mp, radius, grad_partials[0], weights, gain)
    hidden = gather_matmul(n, feats, gains[:, 0].reshape(1, -1), perturbed)
    return (hidden, perturbed)


def grid_kernel(
    n_mp, radius, x_ref, gain_ref, g_ref, w_ref, hid_out, w_out,
    part0, part1, recv0, recv1, own0, own1, grad, sq0, sq1, wnew, hid, near, far,
    turned, zstat, stat, sums,
    push_send, push_recv, hop_send, hop_recv, own_sem, load_sem, store_sem,
    z_send, z_recv, stat_send, stat_recv, sums_send, sums_recv,
    cross_send, cross_recv, relay_send, relay_recv, spread_send, spread_recv,
    y_send, y_recv, mine_send, mine_recv, pass_send, pass_recv, c_send, c_recv,
):
    part, recv, own, sq = (part0, part1), (recv0, recv1), (own0, own1), (sq0, sq1)
    me, z = lax.axis_index("dp"), lax.axis_index("mp")
    core, x, y = me % 2, (me // 2) % 2, me // 4
    rows, width = part0.shape[1], (part0.shape[2], part1.shape[2])
    start_col = (0, width[0])
    sub, tile, tokens, feats = rows // SUBS, 16, hid.shape[0], near.shape[2]
    chunks = (width[0] // CHUNK, width[1] // CHUNK)

    def device(flip_x, flip_y, which):
        cx = 1 - x if flip_x else x
        cy = 1 - y if flip_y else y
        return (cy * 2 + cx) * 2 + which

    partner, x_peer, y_peer = device(0, 0, 1 - core), device(1, 0, core), device(0, 1, core)
    flips = (((1, 1), (1, 0), (0, 1), (0, 0)), ((1, 1), (0, 1), (1, 0), (0, 0)))
    hops = ((x_peer, x_peer, y_peer), (y_peer, y_peer, x_peer))
    dp_peers, mp_peers = others("dp", 8), others("mp", n_mp)

    def span(i, size):
        return pl.ds(pl.multiple_of(i * size, size), size)

    def block(s, i, d, which):
        start = device(*flips[d][s], which) * rows + i * sub
        return g_ref.at[pl.ds(pl.multiple_of(start, tile), sub), pl.ds(start_col[d], width[d])]

    def piece(ref, s, i):
        return ref.at[s, span(i, sub)]

    def push(s, i, d):
        at = (s * SUBS + i) * 2 + d
        return remote(
            block(s, i, d, 1 - core), piece(part[d], s, i), push_send.at[at], push_recv.at[at], partner
        )

    def load(s, i, d, slot):
        return pltpu.make_async_copy(block(s, i, d, core), own[d].at[slot], own_sem.at[slot * 2 + d])

    def hop(s, i, d):
        at = (s * SUBS + i) * 2 + d
        return remote(
            piece(part[d], s, i), piece(recv[d], s, i), hop_send.at[at], hop_recv.at[at], hops[d][s]
        )

    def add(s, i, slot):
        for d in range(2):
            load(s, i, d, slot).wait()
            push(s, i, d).wait_recv()
            came = {0: (), 1: (), 2: (0,), 3: (1, 2)}[s]
            for k in came:
                hop(k, i, d).wait_recv()
            source, mine = piece(part[d], s, i), own[d].at[slot]
            extra = [piece(recv[d], k, i) for k in came]

            @pl.loop(0, sub // tile)
            def _(r):
                at = span(r, tile)
                value = mine[at, :].astype(jnp.float32) + source[at, :].astype(jnp.float32)
                for ref in extra:
                    value = value + ref[at, :].astype(jnp.float32)
                if s == 3:
                    row = pl.multiple_of(i * sub + r * tile, tile)
                    grad[pl.ds(row, tile), start_col[d] : start_col[d] + width[d]] = value
                    squared = value * value
                    sq[d][...] += squared[:8] + squared[8:]
                else:
                    source[at, :] = value.astype(jnp.bfloat16)

            if s < 3:
                hop(s, i, d).start()

    def both(make, *args):
        for d in range(2):
            make(*args[:2], d, *args[2:]).start()

    fetch = pltpu.make_async_copy(x_ref, hid.at[:, pl.ds(0, feats)], load_sem.at[0])
    fetch_w = pltpu.make_async_copy(w_ref, wnew, load_sem.at[1])
    tall, lines = turned.shape[1], 64

    def z_copy(k):
        return remote(
            zstat.at[z], zstat.at[z], z_send.at[k], z_recv.at[k], (z + k + 1) % n_mp, "mp"
        )

    def gather_statistics():
        fetch.wait()

        @pl.loop(0, tokens // tall)
        def _(b):
            @pl.loop(0, tall // lines)
            def _(r):
                at = pl.ds(pl.multiple_of(b * tall + r * lines, lines), lines)
                values = hid[at, :feats].astype(jnp.float32)
                center = jnp.mean(values, axis=1, keepdims=True)
                moved = values - center
                spread = jnp.sum(moved * moved, axis=1, keepdims=True)
                turned[0, span(r, lines), :] = jnp.broadcast_to(center, (lines, tall))
                turned[1, span(r, lines), :] = jnp.broadcast_to(spread, (lines, tall))

            for k in range(2):
                zstat[z, k, b] = turned[k].T[:8]

    belongs = (z + x) % 2 == 0
    half = tokens // 2

    def cross_copy(send):
        src = hid.at[pl.ds(0, half), pl.ds(0, feats)] if send == 0 else relay_room
        return remote(
            src, far.at[z // 2, pl.ds(send * half, half)], cross_send.at[0], cross_recv.at[0], x_peer
        )

    relay_room = hid.at[pl.ds(0, half), pl.ds(feats, feats)]
    relay_copy = remote(
        hid.at[pl.ds(half, half), pl.ds(0, feats)], relay_room,
        relay_send.at[0], relay_recv.at[0], z + 1 - 2 * (z % 2), "mp",
    )

    items = [(x + 2 * k, near.at[k, pl.ds(0, half)]) for k in range(2)]
    items += [(x + 2 * k, near.at[k, pl.ds(half, half)]) for k in range(2)]
    items += [(x + 2 * k, far.at[k, pl.ds(0, half)]) for k in range(2)]
    items += [(1 - x + 2 * k, far.at[k, pl.ds(half, half)]) for k in range(2)]
    near_top, near_low, far_top, far_low = (0, 1), (2, 3), (4, 5), (6, 7)

    def spread_copy(k, way):
        return remote(
            items[k][1], items[k][1], spread_send.at[k * 2 + way], spread_recv.at[k],
            z + 1 - 2 * way, "mp",
        )

    def spread(which, steps):
        for k in which:
            away = z - items[k][0]
            if steps == 0 and k >= 4:

                @pl.when(away == 0)
                def _():
                    cross_copy(0).wait_recv()

            for way, sign in ((0, 1), (1, -1)):
                @pl.when((away * sign == steps) & ((z < n_mp - 1) if way == 0 else (z > 0)))
                def _():
                    if steps > 0:
                        spread_copy(k, way).wait_recv()
                    spread_copy(k, way).start()

    def spread_arrived(which):
        for k in which:
            away = z - items[k][0]

            @pl.when(((z == 0) & (away < 0)) | ((z == n_mp - 1) & (away > 0)))
            def _():
                spread_copy(k, 0).wait_recv()

    def spread_sent():
        for k in range(8):
            away = z - items[k][0]

            @pl.when((away >= 0) & (z < n_mp - 1))
            def _():
                spread_copy(k, 0).wait_send()

            @pl.when((away <= 0) & (z > 0))
            def _():
                spread_copy(k, 1).wait_send()

        cross_copy(0).wait_send()

        @pl.when((z + x) % 2 == 1)
        def _():
            relay_copy.wait_send()

    def normalise():
        for k in range(n_mp - 1):
            z_copy(k).wait_recv()
        centers = [zstat[k, 0] for k in range(n_mp)]
        center = sum(centers) * (1.0 / n_mp)
        squared = sum(zstat[k, 1] for k in range(n_mp))
        squared = squared + feats * sum((one - center) * (one - center) for one in centers)
        scaled = 1.0 / jnp.sqrt(squared * (1.0 / (feats * n_mp)) + 1e-06)
        for k in range(n_mp - 1):
            z_copy(k).wait_send()
        zstat[0, 0] = center
        zstat[0, 1] = scaled

        @pl.loop(0, tokens // tall)
        def _(b):
            for k in range(2):
                turned[k] = jnp.broadcast_to(zstat[0, k, b][:1], (tall, tall)).T

            @pl.loop(0, tall // lines)
            def _(r):
                at = pl.ds(pl.multiple_of(b * tall + r * lines, lines), lines)
                values = hid[at, :feats].astype(jnp.float32)
                moved = values - turned[0, span(r, lines), :1]
                value = moved * turned[1, span(r, lines), :1] * gain_ref[...].astype(jnp.float32)
                value = value.astype(jnp.bfloat16)
                hid[at, :feats] = value

                @pl.when(belongs)
                def _():
                    near[z // 2, at, :] = value

        @pl.when((z + x) % 2 == 1)
        def _():
            cross_copy(0).start()
            relay_copy.start()

        spread(near_top + near_low, 0)

    def relay():
        @pl.when(belongs)
        def _():
            relay_copy.wait_recv()
            cross_copy(1).start()

    def events(i, table):
        for k, actions in table.items():
            @pl.when(i == k)
            def _():
                for action in actions:
                    action()

    def later(which, steps):
        return lambda: spread(which, steps)

    fetch.start()
    both(load, 0, 0, 0)
    sq0[...] = jnp.zeros_like(sq0)
    sq1[...] = jnp.zeros_like(sq1)
    greet(dp_peers + mp_peers, gather_statistics)

    @pl.loop(0, SUBS)
    def _(i):
        both(push, 0, i)

    for k in range(n_mp - 1):
        z_copy(k).start()

    @pl.loop(0, SUBS)
    def _(i):
        @pl.when(i + 1 < SUBS)
        def _():
            both(load, 0, i + 1, (i + 1) % 2)

        @pl.when(i + 1 == SUBS)
        def _():
            both(load, 1, 0, 0)

        both(push, 1, i)
        both(push, 2, i)
        add(0, i, i % 2)
        events(i, {1: [normalise]})

    @pl.loop(0, SUBS)
    def _(i):
        both(load, 2, i, 1)
        both(push, 3, i)
        add(1, i, 0)

        @pl.when(i + 1 < SUBS)
        def _():
            both(load, 1, i + 1, 0)

        @pl.when(i + 1 == SUBS)
        def _():
            both(load, 3, 0, 0)

        add(2, i, 1)
        events(i, {0: [relay], 3: [later(near_top, 1)]})

    fetch_w.start()
    spread(far_top, 0)
    spread(near_low, 1)

    @pl.loop(0, SUBS)
    def _(i):
        @pl.when(i + 1 < SUBS)
        def _():
            both(load, 3, i + 1, (i + 1) % 2)

        add(3, i, i % 2)
        events(
            i,
            {
                0: [later(far_low, 0), later(near_top, 2)],
                1: [later(far_top, 1)],
                2: [later(far_low, 1)],
                3: [later(far_top, 2), later(far_low, 2)],
            },
        )

    folded = jnp.zeros((8, 128), jnp.float32)
    for d in range(2):
        for c in range(width[d] // 128):
            folded = folded + sq[d][:, c * 128 : (c + 1) * 128]
    stat[0] = folded

    @pl.loop(0, SUBS)
    def _(i):
        for d in range(2):
            for s in range(4):
                push(s, i, d).wait_send()
            for s in range(3):
                hop(s, i, d).wait_send()

    def share(slots, peers, send, arrive):
        copies = [
            remote(slots.at[0], slots.at[k + 1], send.at[k], arrive.at[k], peer, axis)
            for k, (axis, peer) in enumerate(peers)
        ]
        for copy in copies:
            copy.start()
        for copy in copies:
            copy.wait()
        return jnp.sum(slots[...], axis=0)

    sums[0] = share(stat, dp_peers, stat_send, stat_recv)
    fetch_w.wait()
    every = share(sums, mp_peers, sums_send, sums_recv)
    squares = jnp.sum(jnp.sum(every, axis=0, keepdims=True), axis=1, keepdims=True)
    scale = radius / jnp.sqrt(squares + 1e-12)

    mine, ours = 2 * y + core, 2 * y + 1 - core
    theirs, others_there = 2 * (1 - y) + core, 2 * (1 - y) + 1 - core

    def slab(d, slot, j):
        return part[d].at[slot, :, span(j, CHUNK)]

    def across(d, j):
        at = d * chunks[0] + j
        here = slab(d, mine, j)
        return remote(here, here, y_send.at[at], y_recv.at[at], y_peer)

    def across_arrived(d, j):
        at = d * chunks[0] + j
        here = slab(d, theirs, j)
        return remote(here, here, y_send.at[at], y_recv.at[at], y_peer)

    def give(d, j, slot):
        at = d * chunks[0] + j
        here = slab(d, mine if slot == "mine" else theirs, j)
        sems = (mine_send, mine_recv) if slot == "mine" else (pass_send, pass_recv)
        return remote(here, here, sems[0].at[at], sems[1].at[at], partner)

    def given(d, j, slot):
        at = d * chunks[0] + j
        here = slab(d, ours if slot == "mine" else others_there, j)
        sems = (mine_send, mine_recv) if slot == "mine" else (pass_send, pass_recv)
        return remote(here, here, sems[0].at[at], sems[1].at[at], partner)

    def partial_copy(d, j):
        at = d * chunks[0] + j
        return remote(
            recv[d].at[0, :, span(j, CHUNK)], recv[d].at[1, :, span(j, CHUNK)],
            c_send.at[at], c_recv.at[at], x_peer,
        )

    def columns(d, j):
        return pl.ds(pl.multiple_of(start_col[d] + j * CHUNK, 128), CHUNK)

    def hid_store(d, j):
        at = d * chunks[0] + j
        cols = columns(d, j)
        return pltpu.make_async_copy(hid.at[:, cols], hid_out.at[:, cols], store_sem.at[at])

    for d in range(2):
        @pl.loop(0, chunks[d])
        def _(j):
            cols = columns(d, j)

            @pl.loop(0, rows // 64)
            def _(r):
                at = span(r, 64)
                value = wnew[at, cols].astype(jnp.float32) + scale * grad[at, cols]
                value = value.astype(jnp.bfloat16)
                wnew[at, cols] = value
                part[d][mine, at, span(j, CHUNK)] = value

            across(d, j).start()
            give(d, j, "mine").start()

    keep = pltpu.make_async_copy(wnew, w_out, load_sem.at[2])
    keep.start()

    def product(left, d, j, size):
        total = None
        for k in range(2):
            right = part[d][2 * k : 2 * k + 2, :, span(j, size)].reshape(2 * rows, size)
            one = jnp.dot(left[k], right, preferred_element_type=jnp.float32)
            total = one if total is None else total + one
        return total

    def arrive(d, j):
        across_arrived(d, j).wait_recv()
        give(d, j, "theirs").start()

    def send_far(d, j):
        given(d, j, "mine").wait_recv()
        given(d, j, "theirs").wait_recv()
        recv[d][0, :, span(j, CHUNK)] = product(far, d, j, CHUNK).astype(jnp.bfloat16)
        partial_copy(d, j).start()

    def keep_near(d, g):
        size = GROUP * CHUNK
        cols = pl.ds(pl.multiple_of(start_col[d] + g * size, 128), size)
        grad[:, cols] = product(near, d, g, size)

    def finish(d, j):
        cols = columns(d, j)
        partial_copy(d, j).wait_recv()

        @pl.loop(0, tokens // 64)
        def _(r):
            at = span(r, 64)
            pre = grad[at, cols] + recv[d][1, at, span(j, CHUNK)].astype(jnp.float32)
            value = 0.5 * pre * (1.0 + lax.erf(pre * math.sqrt(0.5)))
            hid[at, cols] = value.astype(jnp.bfloat16)

        hid_store(d, j).start()

    spread(near_low, 2)
    spread_arrived(far_top + far_low)

    @pl.loop(0, chunks[0])
    def _(j):
        arrive(0, j)
        send_far(0, j)

    spread_arrived(near_top + near_low)
    spread_sent()

    @pl.loop(0, chunks[1])
    def _(j):
        arrive(1, j)

        @pl.when(j < chunks[0] // GROUP)
        def _():
            keep_near(0, j)
            for k in range(GROUP):
                finish(0, j * GROUP + k)

        @pl.when(j >= GROUP)
        def _():
            finish(1, j - GROUP)

        send_far(1, j)

        @pl.when(j % GROUP == GROUP - 1)
        def _():
            keep_near(1, j // GROUP)

    for j in range(chunks[1] - GROUP, chunks[1]):
        finish(1, j)

    keep.wait()
    for d in range(2):
        @pl.loop(0, chunks[d])
        def _(j):
            across(d, j).wait_send()
            give(d, j, "mine").wait_send()
            give(d, j, "theirs").wait_send()
            partial_copy(d, j).wait_send()
            hid_store(d, j).wait()


def grid_program(n_mp, radius, tokens, gain, weights, grads):
    depth, cols = grads.shape
    rows = depth // 8
    count, feats = tokens.shape
    unit = GROUP * CHUNK
    first = cols * 3 // 8 // unit * unit
    wide = (first, cols - first)
    sub, pieces = rows // SUBS, cols // CHUNK
    dma = pltpu.SemaphoreType.DMA
    bf16, f32 = jnp.bfloat16, jnp.float32
    anywhere = pl.BlockSpec(memory_space=pl.ANY)
    return pl.pallas_call(
        functools.partial(grid_kernel, n_mp, radius),
        out_shape=(
            jax.ShapeDtypeStruct((count, cols), bf16),
            jax.ShapeDtypeStruct((rows, cols), bf16),
        ),
        in_specs=[anywhere, pl.BlockSpec(memory_space=pltpu.VMEM), anywhere, anywhere],
        out_specs=(anywhere, anywhere),
        scratch_shapes=[
            pltpu.VMEM((4, rows, wide[0]), bf16),
            pltpu.VMEM((4, rows, wide[1]), bf16),
            pltpu.VMEM((3, rows, wide[0]), bf16),
            pltpu.VMEM((3, rows, wide[1]), bf16),
            pltpu.VMEM((2, sub, wide[0]), bf16),
            pltpu.VMEM((2, sub, wide[1]), bf16),
            pltpu.VMEM((rows, cols), f32),
            pltpu.VMEM((8, wide[0]), f32),
            pltpu.VMEM((8, wide[1]), f32),
            pltpu.VMEM((rows, cols), bf16),
            pltpu.VMEM((count, cols), bf16),
            pltpu.VMEM((2, count, feats), bf16),
            pltpu.VMEM((2, count, feats), bf16),
            pltpu.VMEM((2, 128, 128), f32),
            pltpu.VMEM((n_mp, 2, count // 128, 8, 128), f32),
            pltpu.VMEM((8, 8, 128), f32),
            pltpu.VMEM((n_mp, 8, 128), f32),
            dma((8 * SUBS,)),
            dma((8 * SUBS,)),
            dma((6 * SUBS,)),
            dma((6 * SUBS,)),
            dma((4,)),
            dma((3,)),
            dma((pieces,)),
            dma((n_mp - 1,)),
            dma((n_mp - 1,)),
            dma((7,)),
            dma((7,)),
            dma((n_mp - 1,)),
            dma((n_mp - 1,)),
            dma((1,)),
            dma((1,)),
            dma((1,)),
            dma((1,)),
            dma((16,)),
            dma((8,)),
        ]
        + [dma((pieces,))] * 8,
        compiler_params=pltpu.CompilerParams(
            collective_id=3, has_side_effects=True, vmem_limit_bytes=67043328
        ),
        name="grid_program",
    )(tokens, gain, grads, weights)


def per_device(n, n_mp, width, tokens, ln_gain, weights, grad_partials):
    radius = 0.7 * math.sqrt(width)
    if n == 4 and n_mp == 4 and weights.shape[1] % (8 * GROUP * CHUNK) == 0:
        return grid_program(n_mp, radius, tokens, ln_gain.reshape(1, -1), weights, grad_partials[0])
    return ring_program(n, n_mp, radius, tokens, ln_gain, weights, grad_partials)


def solution(mesh):
    placed = (P("dp", "mp"), P("mp"), P("dp", "mp"), P("dp", None, "mp"))

    def whole(tokens, ln_gain, weights, grad_partials):
        return jax.shard_map(
            functools.partial(per_device, mesh.shape["dp"] // 2, mesh.shape["mp"], weights.shape[1]),
            mesh=mesh,
            in_specs=placed,
            out_specs=(P("dp", "mp"), P("dp", "mp")),
            check_vma=False,
        )(tokens, ln_gain, weights, grad_partials)

    return whole
```

```python
import functools
import math

import jax
import jax.numpy as jnp
from jax import lax
from jax.experimental import pallas as pl
from jax.experimental.pallas import tpu as pltpu
from jax.sharding import PartitionSpec as P

SUBS = 6
AHEAD = 2
CHUNK = 128
GROUP = 3
VMEM_LIMIT = 66 * 1000 * 1000


def power_of_two(n):
    return n & (n - 1) == 0


def chip_at(pos, n):
    if not power_of_two(n):
        return pos
    bits = n.bit_length() - 1
    out = 0
    for b in range(bits):
        out = out + ((pos // 2**b + pos // 2 ** (b + 1)) % 2) * 2**b
    return out


def position_of(chip, n):
    if not power_of_two(n):
        return chip
    bits = n.bit_length() - 1
    above, out = 0, 0
    for b in reversed(range(bits)):
        above = (chip // 2**b + above) % 2
        out = out + above * 2**b
    return out


def ring(n):
    me = lax.axis_index("dp")
    chip, core = me // 2, me % 2
    pos = position_of(chip, n)
    right = chip_at((pos + 1) % n, n) * 2 + core
    left = chip_at((pos + n - 1) % n, n) * 2 + core
    return pos, core, (right, left), chip * 2 + 1 - core


def greet(peers):
    barrier = pltpu.get_barrier_semaphore()
    for device_id in peers:
        pl.semaphore_signal(
            barrier, inc=1, device_id=device_id, device_id_type=pl.DeviceIdType.MESH
        )
    pl.semaphore_wait(barrier, len(peers))


def others(axis, size):
    me = lax.axis_index(axis)
    return [(axis, (me + k) % size) for k in range(1, size)]


def remote(src, dst, send, recv, peer, axis="dp"):
    return pltpu.make_async_remote_copy(
        src_ref=src,
        dst_ref=dst,
        send_sem=send,
        recv_sem=recv,
        device_id={axis: peer},
        device_id_type=pl.DeviceIdType.MESH,
    )


def scatter_kernel(
    n, n_mp, radius, g_ref, w_ref, gain_ref, out_ref, gains_ref,
    part, recv, own, grad, sq_ref, stat, sums, gains,
    part_send, part_recv, hop_send, hop_recv, own_sem,
    stat_send, stat_recv, sums_send, sums_recv, gain_send, gain_recv,
):
    pos, core, hops, partner = ring(n)
    rows, half = part.shape[2], part.shape[3]
    sub = rows // SUBS
    total = n * SUBS
    tile = 16
    dp_peers, mp_peers = others("dp", 2 * n), others("mp", n_mp)
    greet([{axis: peer} for axis, peer in dp_peers + mp_peers])

    def block(t, d, which):
        s, i = t // SUBS, t % SUBS
        target = (pos + n - 1 - s + n) % n if d == 0 else (pos + 1 + s) % n
        start = (chip_at(target, n) * 2 + which) * rows + i * sub
        return g_ref.at[pl.ds(pl.multiple_of(start, tile), sub), pl.ds(d * half, half)]

    def piece(ref, t, d):
        return ref.at[t // SUBS, d, pl.ds(pl.multiple_of((t % SUBS) * sub, tile), sub)]

    def push(t, d):
        at = t * 2 + d
        return remote(
            block(t, d, 1 - core), piece(part, t, d), part_send.at[at], part_recv.at[at], partner
        )

    def load(t, d):
        return pltpu.make_async_copy(block(t, d, core), own.at[t % 2, d], own_sem.at[(t % 2) * 2 + d])

    def hop(t, d, src):
        at = t * 2 + d
        return remote(piece(src, t, d), piece(recv, t, d), hop_send.at[at], hop_recv.at[at], hops[d])

    for d in range(2):
        load(0, d).start()

    @pl.loop(0, SUBS)
    def _(t):
        for d in range(2):
            push(t, d).start()

    place = lax.axis_index("mp")
    fetch = pltpu.make_async_copy(w_ref, out_ref, own_sem.at[4])
    fetch.start()
    gain_copies = [
        remote(gain_ref, gains.at[place], gain_send.at[k], gain_recv.at[k], peer, axis)
        for k, (axis, peer) in enumerate(mp_peers)
    ]
    for copy in gain_copies:
        copy.start()
    gains[place] = gain_ref[...]
    sq_ref[...] = jnp.zeros_like(sq_ref)

    def step(t, first, last):
        @pl.when(t + 1 < total)
        def _():
            for d in range(2):
                load(t + 1, d).start()

        @pl.when(t + SUBS < total)
        def _():
            for d in range(2):
                push(t + SUBS, d).start()

        for d in range(2):
            load(t, d).wait()
            push(t, d).wait_recv()
            if not first:
                hop(t - SUBS, d, recv).wait_recv()
            source = piece(part, t, d)
            came = None if first else piece(recv, t - SUBS, d)
            mine = own.at[t % 2, d]

            @pl.loop(0, sub // tile)
            def _(r):
                at = pl.ds(pl.multiple_of(r * tile, tile), tile)
                value = mine[at, :].astype(jnp.float32) + source[at, :].astype(jnp.float32)
                if not first:
                    value = value + came[at, :].astype(jnp.float32)
                if last:
                    row = pl.multiple_of((t % SUBS) * sub + r * tile, tile)
                    grad[pl.ds(row, tile), d * half : (d + 1) * half] = value
                    squared = value * value
                    sq_ref[...] += squared[:8] + squared[8:]
                elif first:
                    source[at, :] = value.astype(jnp.bfloat16)
                else:
                    came[at, :] = value.astype(jnp.bfloat16)

        if not last:
            for d in range(2):
                at = t * 2 + d
                src = piece(part, t, d) if first else piece(recv, t - SUBS, d)
                remote(src, piece(recv, t, d), hop_send.at[at], hop_recv.at[at], hops[d]).start()

    @pl.loop(0, SUBS)
    def _(t):
        step(t, True, False)

    @pl.loop(SUBS, total - SUBS)
    def _(t):
        step(t, False, False)

    @pl.loop(total - SUBS, total)
    def _(t):
        step(t, False, True)

    folded = sq_ref[:, :128]
    for c in range(1, half // 128):
        folded = folded + sq_ref[:, c * 128 : (c + 1) * 128]
    stat[0] = folded

    @pl.loop(0, total)
    def _(t):
        for d in range(2):
            push(t, d).wait_send()

    @pl.loop(0, total - SUBS)
    def _(t):
        for d in range(2):
            hop(t, d, recv).wait_send()

    def share(slots, peers, send, arrive):
        copies = [
            remote(slots.at[0], slots.at[k + 1], send.at[k], arrive.at[k], peer, axis)
            for k, (axis, peer) in enumerate(peers)
        ]
        for copy in copies:
            copy.start()
        for copy in copies:
            copy.wait()
        return jnp.sum(slots[...], axis=0)

    sums[0] = share(stat, dp_peers, stat_send, stat_recv)
    for copy in gain_copies:
        copy.wait()
    gains_ref[...] = gains[...]
    fetch.wait()
    every = share(sums, mp_peers, sums_send, sums_recv)
    squares = jnp.sum(jnp.sum(every, axis=0, keepdims=True), axis=1, keepdims=True)
    scale = radius / jnp.sqrt(squares + 1e-12)

    @pl.loop(0, rows // tile)
    def _(r):
        at = pl.ds(pl.multiple_of(r * tile, tile), tile)
        value = out_ref[at, :].astype(jnp.float32) + scale * grad[at, :]
        out_ref[at, :] = value.astype(jnp.bfloat16)


def reduce_rows(n, n_mp, radius, grads, weights, gain):
    depth, cols = grads.shape
    rows, half = depth // (2 * n), cols // 2
    sub = rows // SUBS
    dma = pltpu.SemaphoreType.DMA
    return pl.pallas_call(
        functools.partial(scatter_kernel, n, n_mp, radius),
        out_shape=(
            jax.ShapeDtypeStruct((rows, cols), jnp.bfloat16),
            jax.ShapeDtypeStruct((n_mp, *gain.shape), jnp.float32),
        ),
        in_specs=[
            pl.BlockSpec(memory_space=pl.ANY),
            pl.BlockSpec(memory_space=pl.ANY),
            pl.BlockSpec(memory_space=pltpu.VMEM),
        ],
        out_specs=(
            pl.BlockSpec(memory_space=pltpu.VMEM),
            pl.BlockSpec(memory_space=pltpu.VMEM),
        ),
        scratch_shapes=[
            pltpu.VMEM((n, 2, rows, half), jnp.bfloat16),
            pltpu.VMEM((n - 1, 2, rows, half), jnp.bfloat16),
            pltpu.VMEM((2, 2, sub, half), jnp.bfloat16),
            pltpu.VMEM((rows, cols), jnp.float32),
            pltpu.VMEM((8, half), jnp.float32),
            pltpu.VMEM((2 * n, 8, 128), jnp.float32),
            pltpu.VMEM((n_mp, 8, 128), jnp.float32),
            pltpu.VMEM((n_mp, *gain.shape), jnp.float32),
            dma((n * SUBS * 2,)),
            dma((n * SUBS * 2,)),
            dma(((n - 1) * SUBS * 2,)),
            dma(((n - 1) * SUBS * 2,)),
            dma((5,)),
            dma((2 * n - 1,)),
            dma((2 * n - 1,)),
            dma((n_mp - 1,)),
            dma((n_mp - 1,)),
            dma((n_mp - 1,)),
            dma((n_mp - 1,)),
        ],
        compiler_params=pltpu.CompilerParams(
            collective_id=1, has_side_effects=True, vmem_limit_bytes=VMEM_LIMIT
        ),
        cost_estimate=pl.CostEstimate(
            flops=200 * 10**9, bytes_accessed=3 * grads.size, transcendentals=0
        ),
        name="reduce_rows",
    )(grads, weights, gain)


def gather_kernel(
    n, x_ref, gain_ref, p_ref, out_ref, normed, buf, pre_ref,
    hop_send, hop_recv, part_send, part_recv, own_sem, x_sem,
):
    pos, core, hops, partner = ring(n)
    rows, width = buf.shape[3] // 2, buf.shape[4]
    half = SUBS * width
    greet([{"dp": peer} for peer in (*hops, partner)])

    def mine(i, d):
        return p_ref.at[:, pl.ds(pl.multiple_of(d * half + i * width, 128), width)]

    def piece(s, i, d, which):
        return buf.at[s, d, i, pl.ds(pl.multiple_of(which * rows, 16), rows)]

    def hop(s, i, d, src):
        at = ((s - 1) * SUBS + i) * 2 + d
        return remote(src, piece(s, i, d, core), hop_send.at[at], hop_recv.at[at], hops[d])

    def push(s, i, d, src):
        at = (s * SUBS + i) * 2 + d
        return remote(src, piece(s, i, d, core), part_send.at[at], part_recv.at[at], partner)

    def pushed(s, i, d):
        at = (s * SUBS + i) * 2 + d
        there = piece(s, i, d, 1 - core)
        return remote(there, there, part_send.at[at], part_recv.at[at], partner)

    def keep(i, d):
        return pltpu.make_async_copy(mine(i, d), piece(0, i, d, core), own_sem.at[i * 2 + d])

    fetch = pltpu.make_async_copy(x_ref, normed, x_sem.at[0])
    fetch.start()
    for i in range(AHEAD):
        for d in range(2):
            hop(1, i, d, mine(i, d)).start()

    @pl.loop(0, SUBS)
    def _(i):
        for d in range(2):
            keep(i, d).start()
            push(0, i, d, mine(i, d)).start()

    pre_ref[...] = jnp.zeros_like(pre_ref)
    fetch.wait()

    @pl.loop(0, normed.shape[0] // 16)
    def _(r):
        at = pl.ds(pl.multiple_of(r * 16, 16), 16)
        values = normed[at, :].astype(jnp.float32)
        center = jnp.mean(values, axis=1, keepdims=True)
        moved = values - center
        spread = jnp.mean(moved * moved, axis=1, keepdims=True)
        scaled = moved * (1.0 / jnp.sqrt(spread + 1e-06)) * gain_ref[...]
        normed[at, :] = scaled.astype(jnp.bfloat16)

    def multiply(s, i):
        for d in range(2):
            pushed(s, i, d).wait_recv()
            owner = (pos + n - s) % n if d == 0 else (pos + s) % n
            cols = pl.ds(pl.multiple_of(chip_at(owner, n) * 2 * rows, 128), 2 * rows)
            out = pl.ds(pl.multiple_of(d * half + i * width, 128), width)
            pre_ref[:, out] += jnp.dot(
                normed[:, cols], buf[s, d, i], preferred_element_type=jnp.float32
            )

    def activate(i):
        tall = 64
        for d in range(2):
            cols = pl.ds(pl.multiple_of(d * half + i * width, 128), width)

            @pl.loop(0, pre_ref.shape[0] // tall)
            def _(r):
                at = pl.ds(pl.multiple_of(r * tall, tall), tall)
                pre = pre_ref[at, cols]
                value = 0.5 * pre * (1.0 + lax.erf(pre * math.sqrt(0.5)))
                out_ref[at, cols] = value.astype(jnp.bfloat16)

    @pl.loop(0, SUBS + n - 1)
    def _(wave):
        @pl.when(wave + AHEAD < SUBS)
        def _():
            for d in range(2):
                hop(1, wave + AHEAD, d, mine(wave + AHEAD, d)).start()

        for s in range(1, n):
            i = wave - (s - 1)

            @pl.when((i >= 0) & (i < SUBS))
            def _():
                for d in range(2):
                    hop(s, i, d, piece(s, i, d, core)).wait_recv()
                    if s < n - 1:
                        hop(s + 1, i, d, piece(s, i, d, core)).start()
                    push(s, i, d, piece(s, i, d, core)).start()

            if s == 1:

                @pl.when(wave < SUBS)
                def _():
                    for d in range(2):
                        keep(wave, d).wait()
                    multiply(0, wave)

            @pl.when((i >= 1) & (i <= SUBS))
            def _():
                multiply(s, i - 1)
                if s == n - 1:
                    activate(i - 1)

    @pl.loop(0, SUBS)
    def _(i):
        for d in range(2):
            for s in range(n):
                push(s, i, d, piece(s, i, d, core)).wait_send()
            for s in range(1, n):
                hop(s, i, d, piece(s, i, d, core)).wait_send()


def gather_matmul(n, feats, gains, perturbed):
    tokens, depth = feats.shape
    rows, cols = perturbed.shape
    half = cols // 2
    dma = pltpu.SemaphoreType.DMA
    return pl.pallas_call(
        functools.partial(gather_kernel, n),
        out_shape=jax.ShapeDtypeStruct((tokens, cols), jnp.bfloat16),
        in_specs=[
            pl.BlockSpec(memory_space=pl.ANY),
            pl.BlockSpec(memory_space=pltpu.VMEM),
            pl.BlockSpec(memory_space=pl.ANY),
        ],
        out_specs=pl.BlockSpec(memory_space=pltpu.VMEM),
        scratch_shapes=[
            pltpu.VMEM((tokens, depth), jnp.bfloat16),
            pltpu.VMEM((n, 2, SUBS, 2 * rows, half // SUBS), jnp.bfloat16),
            pltpu.VMEM((tokens, cols), jnp.float32),
            dma(((n - 1) * SUBS * 2,)),
            dma(((n - 1) * SUBS * 2,)),
            dma((n * SUBS * 2,)),
            dma((n * SUBS * 2,)),
            dma((SUBS * 2,)),
            dma((1,)),
        ],
        compiler_params=pltpu.CompilerParams(
            collective_id=2, has_side_effects=True, vmem_limit_bytes=VMEM_LIMIT
        ),
        cost_estimate=pl.CostEstimate(
            flops=2 * tokens * depth * cols,
            bytes_accessed=2 * depth * cols,
            transcendentals=0,
        ),
        name="gather_matmul",
    )(feats, gains, perturbed)


def ring_program(n, n_mp, radius, tokens, ln_gain, weights, grad_partials):
    feats = lax.all_gather(tokens, "mp", axis=1, tiled=True)
    gain = jnp.broadcast_to(ln_gain.astype(jnp.float32), (8, ln_gain.shape[0]))
    perturbed, gains = reduce_rows(n, n_mp, radius, grad_partials[0], weights, gain)
    hidden = gather_matmul(n, feats, gains[:, 0].reshape(1, -1), perturbed)
    return (hidden, perturbed)


def grid_kernel(
    n_mp, radius, x_ref, gain_ref, g_ref, w_ref, hid, wnew,
    part0, part1, recv0, recv1, own0, own1, grad, sq0, sq1, near, far,
    turned, zstat, stat,
    push_send, push_recv, hop_send, hop_recv, own_sem, load_sem,
    z_send, z_recv, stat_send, stat_recv,
    cross_send, cross_recv, relay_send, relay_recv, spread_send, spread_recv,
    y_send, y_recv, mine_send, mine_recv, pass_send, pass_recv, c_send, c_recv,
):
    part, recv, own, sq = (part0, part1), (recv0, recv1), (own0, own1), (sq0, sq1)
    me, z = lax.axis_index("dp"), lax.axis_index("mp")
    core, x, y = me % 2, (me // 2) % 2, me // 4
    rows, width = part0.shape[1], (part0.shape[2], part1.shape[2])
    start_col = (0, width[0])
    sub, tile, tokens, feats = rows // SUBS, 16, hid.shape[0], near.shape[2]
    chunks = (width[0] // CHUNK, width[1] // CHUNK)

    def device(flip_x, flip_y, which):
        cx = 1 - x if flip_x else x
        cy = 1 - y if flip_y else y
        return (cy * 2 + cx) * 2 + which

    partner, x_peer, y_peer = device(0, 0, 1 - core), device(1, 0, core), device(0, 1, core)
    flips = (((1, 1), (1, 0), (0, 1), (0, 0)), ((1, 1), (0, 1), (1, 0), (0, 0)))
    hops = ((x_peer, x_peer, y_peer), (y_peer, y_peer, x_peer))
    everyone = [
        {"dp": (me + a) % 8, "mp": (z + b) % n_mp} for a in range(8) for b in range(n_mp) if a + b
    ]

    def span(i, size):
        return pl.ds(pl.multiple_of(i * size, size), size)

    def block(s, i, d, which):
        start = device(*flips[d][s], which) * rows + i * sub
        return g_ref.at[pl.ds(pl.multiple_of(start, tile), sub), pl.ds(start_col[d], width[d])]

    def piece(ref, s, i):
        return ref.at[s, span(i, sub)]

    def push(s, i, d):
        at = (s * SUBS + i) * 2 + d
        return remote(
            block(s, i, d, 1 - core), piece(part[d], s, i), push_send.at[d], push_recv.at[at], partner
        )

    def load(s, i, d, slot):
        return pltpu.make_async_copy(block(s, i, d, core), own[d].at[slot], own_sem.at[slot * 2 + d])

    def hop(s, i, d):
        at = (s * SUBS + i) * 2 + d
        return remote(
            piece(part[d], s, i), piece(recv[d], s, i), hop_send.at[d], hop_recv.at[at], hops[d][s]
        )

    def add(s, i, slot):
        for d in range(2):
            load(s, i, d, slot).wait()
            push(s, i, d).wait_recv()
            came = {0: (), 1: (), 2: (0,), 3: (1, 2)}[s]
            if s > 1:
                hop(2 * s - 4, i, d).wait_recv()
            source, mine = piece(part[d], s, i), own[d].at[slot]
            extra = [piece(recv[d], k, i) for k in came]

            @pl.loop(0, sub // tile)
            def _(r):
                at = span(r, tile)
                value = mine[at, :].astype(jnp.float32) + source[at, :].astype(jnp.float32)
                for ref in extra:
                    value = value + ref[at, :].astype(jnp.float32)
                if s == 3:
                    row = pl.multiple_of(i * sub + r * tile, tile)
                    grad[pl.ds(row, tile), start_col[d] : start_col[d] + width[d]] = value
                    squared = value * value
                    sq[d][...] += squared[:8] + squared[8:]
                else:
                    source[at, :] = value.astype(jnp.bfloat16)

            if s < 3:
                hop(s, i, d).start()

    def both(make, *args):
        for d in range(2):
            make(*args[:2], d, *args[2:]).start()

    fetch = pltpu.make_async_copy(x_ref, hid.at[:, pl.ds(0, feats)], load_sem.at[0])
    fetch_w = pltpu.make_async_copy(w_ref, wnew, load_sem.at[1])
    tall, lines = turned.shape[1], 64

    def z_copy(k):
        return remote(
            zstat.at[z], zstat.at[z], z_send.at[k], z_recv.at[k], (z + k + 1) % n_mp, "mp"
        )

    def gather_statistics():
        fetch.wait()

        @pl.loop(0, tokens // tall)
        def _(b):
            @pl.loop(0, tall // lines)
            def _(r):
                at = pl.ds(pl.multiple_of(b * tall + r * lines, lines), lines)
                values = hid[at, :feats].astype(jnp.float32)
                center = jnp.mean(values, axis=1, keepdims=True)
                moved = values - center
                spread = jnp.sum(moved * moved, axis=1, keepdims=True)
                turned[0, span(r, lines), :] = jnp.broadcast_to(center, (lines, tall))
                turned[1, span(r, lines), :] = jnp.broadcast_to(spread, (lines, tall))

            for k in range(2):
                zstat[z, k, b] = turned[k].T[:8]

        for k in range(n_mp - 1):
            z_copy(k).start()

    belongs = (z + x) % 2 == 0
    half = tokens // 2

    def cross_copy(send):
        src = hid.at[pl.ds(0, half), pl.ds(0, feats)] if send == 0 else relay_room
        return remote(
            src, far.at[z // 2, pl.ds(send * half, half)], cross_send.at[0], cross_recv.at[0], x_peer
        )

    relay_room = hid.at[pl.ds(0, half), pl.ds(feats, feats)]
    relay_copy = remote(
        hid.at[pl.ds(half, half), pl.ds(0, feats)], relay_room,
        relay_send.at[0], relay_recv.at[0], z + 1 - 2 * (z % 2), "mp",
    )

    ends = ((3 * x, x), (2 - x, 1 - x))
    items = [(o, near.at[k, pl.ds(h * half, half)]) for o, k in ends for h in range(2)]
    items += [(x + 2 * k, far.at[k, pl.ds(0, half)]) for k in range(2)]
    items += [(1 - x + 2 * k, far.at[k, pl.ds(half, half)]) for k in range(2)]
    near_top, long_low, short_low, far_top, far_low = (0, 2), (1,), (3,), (4, 5), (6, 7)

    def spread_copy(k, way):
        return remote(
            items[k][1], items[k][1], spread_send.at[k * 2 + way], spread_recv.at[k],
            z + 1 - 2 * way, "mp",
        )

    def spread(which, steps):
        for k in which:
            away = z - items[k][0]
            if steps == 0 and k >= 4:

                @pl.when(away == 0)
                def _():
                    cross_copy(0).wait_recv()

            for way, sign in ((0, 1), (1, -1)):
                @pl.when((away * sign == steps) & ((z < n_mp - 1) if way == 0 else (z > 0)))
                def _():
                    if steps > 0:
                        spread_copy(k, way).wait_recv()
                    spread_copy(k, way).start()

    def spread_arrived(which):
        for k in which:
            away = z - items[k][0]

            @pl.when(((z == 0) & (away < 0)) | ((z == n_mp - 1) & (away > 0)))
            def _():
                spread_copy(k, 0).wait_recv()

    def spread_sent():
        for k in range(8):
            away = z - items[k][0]

            @pl.when((away >= 0) & (z < n_mp - 1))
            def _():
                spread_copy(k, 0).wait_send()

            @pl.when((away <= 0) & (z > 0))
            def _():
                spread_copy(k, 1).wait_send()

        cross_copy(0).wait_send()

        @pl.when((z + x) % 2 == 1)
        def _():
            relay_copy.wait_send()

    def normalise():
        for k in range(n_mp - 1):
            z_copy(k).wait_recv()
        centers = [zstat[k, 0] for k in range(n_mp)]
        center = sum(centers) * (1.0 / n_mp)
        squared = sum(zstat[k, 1] for k in range(n_mp))
        squared = squared + feats * sum((one - center) * (one - center) for one in centers)
        scaled = 1.0 / jnp.sqrt(squared * (1.0 / (feats * n_mp)) + 1e-06)
        for k in range(n_mp - 1):
            z_copy(k).wait_send()
        zstat[0, 0] = center
        zstat[0, 1] = scaled

        for h in range(2):
            @pl.loop(h * half // tall, (h + 1) * half // tall)
            def _(b):
                for k in range(2):
                    turned[k] = jnp.broadcast_to(zstat[0, k, b][:1], (tall, tall)).T

                @pl.loop(0, tall // lines)
                def _(r):
                    at = pl.ds(pl.multiple_of(b * tall + r * lines, lines), lines)
                    values = hid[at, :feats].astype(jnp.float32)
                    moved = values - turned[0, span(r, lines), :1]
                    value = moved * turned[1, span(r, lines), :1] * gain_ref[...].astype(jnp.float32).reshape(1, feats)
                    value = value.astype(jnp.bfloat16)
                    hid[at, :feats] = value

                    @pl.when(belongs)
                    def _():
                        near[z // 2, at, :] = value

            @pl.when((z + x) % 2 == 1)
            def _():
                (cross_copy(0) if h == 0 else relay_copy).start()

            spread(near_top if h == 0 else long_low + short_low, 0)

    def relay():
        @pl.when(belongs)
        def _():
            relay_copy.wait_recv()
            cross_copy(1).start()

    def events(i, table):
        for k, actions in table.items():
            @pl.when(i == k)
            def _():
                for action in actions:
                    action()

    def later(which, steps):
        return lambda: spread(which, steps)

    fetch.start()
    both(load, 0, 0, 0)
    sq0[...] = jnp.zeros_like(sq0)
    sq1[...] = jnp.zeros_like(sq1)
    greet(everyone)

    @pl.loop(0, SUBS)
    def _(i):
        both(push, 0, i)

    @pl.loop(0, SUBS)
    def _(i):
        @pl.when(i + 1 < SUBS)
        def _():
            both(load, 0, i + 1, (i + 1) % 2)

        @pl.when(i + 1 == SUBS)
        def _():
            both(load, 1, 0, 0)

        both(push, 1, i)
        both(push, 2, i)
        add(0, i, i % 2)
        events(i, {0: [gather_statistics], 2: [normalise]})

    @pl.loop(0, SUBS)
    def _(i):
        both(load, 2, i, 1)
        both(push, 3, i)
        add(1, i, 0)

        @pl.when(i + 1 < SUBS)
        def _():
            both(load, 1, i + 1, 0)

        @pl.when(i + 1 == SUBS)
        def _():
            both(load, 3, 0, 0)

        add(2, i, 1)
        events(
            i,
            {
                0: [relay],
                2: [later(near_top, 1)],
                3: [later(far_top, 0)],
                4: [later(short_low, 1)],
            },
        )

    fetch_w.start()

    @pl.loop(0, SUBS)
    def _(i):
        @pl.when(i + 1 < SUBS)
        def _():
            both(load, 3, i + 1, (i + 1) % 2)

        for d in range(2):
            hop(1, i, d).wait_recv()
        events(
            i,
            {
                0: [later(near_top, 2), later(far_low, 0)],
                3: [later(far_top, 2), later(far_low, 2)],
            },
        )
        add(3, i, i % 2)
        events(i, {0: [later(far_top, 1)], 1: [later(far_low, 1)], 2: [later(long_low, 1)]})

    folded = jnp.zeros((8, 128), jnp.float32)
    for d in range(2):
        for c in range(width[d] // 128):
            folded = folded + sq[d][:, c * 128 : (c + 1) * 128]
    stat[0] = folded

    for d in range(2):
        remote(part[d], part[d], push_send.at[d], push_recv.at[0], partner).wait_send()
        sent = part[d].at[pl.ds(0, 3)]
        remote(sent, recv[d], hop_send.at[d], hop_recv.at[0], partner).wait_send()

    def shared(src, dst, device_id):
        return pltpu.make_async_remote_copy(
            src_ref=src,
            dst_ref=dst,
            send_sem=stat_send.at[0],
            recv_sem=stat_recv.at[0],
            device_id=device_id,
            device_id_type=pl.DeviceIdType.MESH,
        )

    for k, device_id in enumerate(everyone):
        shared(stat.at[pl.ds(0, 1)], stat.at[pl.ds(k + 1, 1)], device_id).start()
    fetch_w.wait()
    rest = stat.at[pl.ds(1, len(everyone))]
    shared(rest, rest, everyone[0]).wait()
    every = jnp.sum(stat[...], axis=0)
    squares = jnp.sum(jnp.sum(every, axis=0, keepdims=True), axis=1, keepdims=True)
    scale = radius / jnp.sqrt(squares + 1e-12)

    mine, ours = 2 * y + core, 2 * y + 1 - core
    theirs, others_there = 2 * (1 - y) + core, 2 * (1 - y) + 1 - core

    def slab(d, slot, j):
        return part[d].at[slot, :, span(j, CHUNK)]

    def across(d, j):
        at = d * chunks[0] + j
        here = slab(d, mine, j)
        return remote(here, here, y_send.at[d], y_recv.at[at], y_peer)

    def across_arrived(d, j):
        at = d * chunks[0] + j
        here = slab(d, theirs, j)
        return remote(here, here, y_send.at[d], y_recv.at[at], y_peer)

    def give(d, j, slot):
        at = d * chunks[0] + j
        here = slab(d, mine if slot == "mine" else theirs, j)
        sems = (mine_send, mine_recv) if slot == "mine" else (pass_send, pass_recv)
        return remote(here, here, sems[0].at[d], sems[1].at[at], partner)

    def given(d, j, slot):
        at = d * chunks[0] + j
        here = slab(d, ours if slot == "mine" else others_there, j)
        sems = (mine_send, mine_recv) if slot == "mine" else (pass_send, pass_recv)
        return remote(here, here, sems[0].at[d], sems[1].at[at], partner)

    def partial_copy(d, j):
        at = d * chunks[0] + j
        return remote(
            recv[d].at[0, :, span(j, CHUNK)], recv[d].at[1, :, span(j, CHUNK)],
            c_send.at[d], c_recv.at[at], x_peer,
        )

    def columns(d, j):
        return pl.ds(pl.multiple_of(start_col[d] + j * CHUNK, 128), CHUNK)

    for d in range(2):
        @pl.loop(0, chunks[d])
        def _(j):
            cols = columns(d, j)

            @pl.loop(0, rows // 64)
            def _(r):
                at = span(r, 64)
                value = wnew[at, cols].astype(jnp.float32) + scale * grad[at, cols]
                value = value.astype(jnp.bfloat16)
                wnew[at, cols] = value
                part[d][mine, at, span(j, CHUNK)] = value

            across(d, j).start()
            give(d, j, "mine").start()

    def product(left, at, d, j, size):
        total = None
        for k in range(2):
            right = part[d][2 * k : 2 * k + 2, :, span(j, size)].reshape(2 * rows, size)
            one = jnp.dot(left[k, at], right, preferred_element_type=jnp.float32)
            total = one if total is None else total + one
        return total

    def arrive(d, j):
        across_arrived(d, j).wait_recv()
        give(d, j, "theirs").start()

    def send_far(d, j):
        given(d, j, "mine").wait_recv()
        given(d, j, "theirs").wait_recv()
        recv[d][0, :, span(j, CHUNK)] = product(far, pl.ds(0, tokens), d, j, CHUNK).astype(jnp.bfloat16)
        partial_copy(d, j).start()

    def keep_near(d, g, h):
        size, at = GROUP * CHUNK, pl.ds(h * half, half)
        cols = pl.ds(pl.multiple_of(start_col[d] + g * size, 128), size)
        grad[at, cols] = product(near, at, d, g, size)

    def settle(d):
        here, there, partial = part[d].at[mine], part[d].at[theirs], recv[d].at[0]
        remote(here, here, y_send.at[d], y_recv.at[0], y_peer).wait_send()
        remote(here, here, mine_send.at[d], mine_recv.at[0], partner).wait_send()
        remote(there, there, pass_send.at[d], pass_recv.at[0], partner).wait_send()
        remote(partial, partial, c_send.at[d], c_recv.at[0], x_peer).wait_send()

    def finish(d, j):
        cols = columns(d, j)
        partial_copy(d, j).wait_recv()

        @pl.loop(0, tokens // 64)
        def _(r):
            at = span(r, 64)
            pre = grad[at, cols] + recv[d][1, at, span(j, CHUNK)].astype(jnp.float32)
            value = 0.5 * pre * (1.0 + lax.erf(pre * math.sqrt(0.5)))
            hid[at, cols] = value.astype(jnp.bfloat16)

    spread(long_low, 2)
    spread_arrived(far_top + far_low)

    @pl.loop(0, chunks[0])
    def _(j):
        arrive(0, j)
        send_far(0, j)

    spread_arrived(near_top + long_low + short_low)
    groups = (chunks[0] // GROUP, chunks[1] // GROUP)
    turns = [0, 1] + [1 + GROUP * k for k in range(1, 2 * groups[0] - 1)]
    spread_sent()

    @pl.loop(0, chunks[1])
    def _(j):
        arrive(1, j)

        @pl.when(j > GROUP)
        def _():
            finish(1, j - GROUP - 1)

        for g in range(groups[0]):
            for k in range(GROUP):
                @pl.when(j == turns[2 * g + 1] + 1 + k)
                def _():
                    finish(0, g * GROUP + k)

        send_far(1, j)

        @pl.when(j % GROUP == GROUP - 1)
        def _():
            keep_near(1, j // GROUP, 0)

        @pl.when((j % GROUP == 0) & (j > 0))
        def _():
            keep_near(1, j // GROUP - 1, 1)

        for k, turn in enumerate(turns):
            @pl.when(j == turn)
            def _():
                keep_near(0, k // 2, k % 2)

    keep_near(1, groups[1] - 1, 1)
    for j in range(max(chunks[1] - turns[-1] - 1, 0), GROUP):
        finish(0, chunks[0] - GROUP + j)
    for j in range(chunks[1] - GROUP - 1, chunks[1]):
        finish(1, j)

    for d in range(2):
        settle(d)


def grid_program(n_mp, radius, tokens, gain, weights, grads):
    depth, cols = grads.shape
    rows = depth // 8
    count, feats = tokens.shape
    unit = GROUP * CHUNK
    first = cols * 3 // 8 // unit * unit
    wide = (first, cols - first)
    sub, pieces = rows // SUBS, cols // CHUNK
    dma = pltpu.SemaphoreType.DMA
    bf16, f32 = jnp.bfloat16, jnp.float32
    anywhere = pl.BlockSpec(memory_space=pl.ANY)
    return pl.pallas_call(
        functools.partial(grid_kernel, n_mp, radius),
        out_shape=(
            pltpu.VMEM((count, cols), bf16),
            pltpu.VMEM((rows, cols), bf16),
        ),
        in_specs=[anywhere, pl.BlockSpec(memory_space=pltpu.VMEM), anywhere, anywhere],
        out_specs=(pl.BlockSpec(memory_space=pltpu.VMEM), pl.BlockSpec(memory_space=pltpu.VMEM)),
        scratch_shapes=[
            pltpu.VMEM((4, rows, wide[0]), bf16),
            pltpu.VMEM((4, rows, wide[1]), bf16),
            pltpu.VMEM((3, rows, wide[0]), bf16),
            pltpu.VMEM((3, rows, wide[1]), bf16),
            pltpu.VMEM((2, sub, wide[0]), bf16),
            pltpu.VMEM((2, sub, wide[1]), bf16),
            pltpu.VMEM((rows, cols), f32),
            pltpu.VMEM((8, wide[0]), f32),
            pltpu.VMEM((8, wide[1]), f32),
            pltpu.VMEM((2, count, feats), bf16),
            pltpu.VMEM((2, count, feats), bf16),
            pltpu.VMEM((2, 128, 128), f32),
            pltpu.VMEM((n_mp, 2, count // 128, 8, 128), f32),
            pltpu.VMEM((8 * n_mp, 8, 128), f32),
            dma((2,)),
            dma((8 * SUBS,)),
            dma((2,)),
            dma((6 * SUBS,)),
            dma((4,)),
            dma((2,)),
            dma((n_mp - 1,)),
            dma((n_mp - 1,)),
            dma((1,)),
            dma((1,)),
            dma((1,)),
            dma((1,)),
            dma((1,)),
            dma((1,)),
            dma((16,)),
            dma((8,)),
        ]
        + [dma((2,)), dma((pieces,))] * 4,
        compiler_params=pltpu.CompilerParams(
            collective_id=3, has_side_effects=True, vmem_limit_bytes=57000000
        ),
        name="grid_program",
    )(tokens, gain, grads, weights)


def per_device(n, n_mp, width, tokens, ln_gain, weights, grad_partials):
    radius = 0.7 * math.sqrt(width)
    if n == 4 and n_mp == 4 and weights.shape[1] % (8 * GROUP * CHUNK) == 0:
        return grid_program(n_mp, radius, tokens, ln_gain, weights, grad_partials[0])
    return ring_program(n, n_mp, radius, tokens, ln_gain, weights, grad_partials)


def solution(mesh):
    placed = (P("dp", "mp"), P("mp"), P("dp", "mp"), P("dp", None, "mp"))

    def whole(tokens, ln_gain, weights, grad_partials):
        return jax.shard_map(
            functools.partial(per_device, mesh.shape["dp"] // 2, mesh.shape["mp"], weights.shape[1]),
            mesh=mesh,
            in_specs=placed,
            out_specs=(P("dp", "mp"), P("dp", "mp")),
            check_vma=False,
        )(tokens, ln_gain, weights, grad_partials)

    return whole
```

```python
import functools
import math

import jax
import jax.numpy as jnp
from jax import lax
from jax.experimental import pallas as pl
from jax.experimental.pallas import tpu as pltpu
from jax.sharding import PartitionSpec as P

SUBS = 6
AHEAD = 2
CHUNK = 128
GROUP = 3
STRIPS = 2
VMEM_LIMIT = 66 * 1000 * 1000


def power_of_two(n):
    return n & (n - 1) == 0


def chip_at(pos, n):
    if not power_of_two(n):
        return pos
    bits = n.bit_length() - 1
    out = 0
    for b in range(bits):
        out = out + ((pos // 2**b + pos // 2 ** (b + 1)) % 2) * 2**b
    return out


def position_of(chip, n):
    if not power_of_two(n):
        return chip
    bits = n.bit_length() - 1
    above, out = 0, 0
    for b in reversed(range(bits)):
        above = (chip // 2**b + above) % 2
        out = out + above * 2**b
    return out


def ring(n):
    me = lax.axis_index("dp")
    chip, core = me // 2, me % 2
    pos = position_of(chip, n)
    right = chip_at((pos + 1) % n, n) * 2 + core
    left = chip_at((pos + n - 1) % n, n) * 2 + core
    return pos, core, (right, left), chip * 2 + 1 - core


def greet(peers):
    barrier = pltpu.get_barrier_semaphore()
    for device_id in peers:
        pl.semaphore_signal(
            barrier, inc=1, device_id=device_id, device_id_type=pl.DeviceIdType.MESH
        )
    pl.semaphore_wait(barrier, len(peers))


def others(axis, size):
    me = lax.axis_index(axis)
    return [(axis, (me + k) % size) for k in range(1, size)]


def remote(src, dst, send, recv, peer, axis="dp"):
    return pltpu.make_async_remote_copy(
        src_ref=src,
        dst_ref=dst,
        send_sem=send,
        recv_sem=recv,
        device_id={axis: peer},
        device_id_type=pl.DeviceIdType.MESH,
    )


def scatter_kernel(
    n, n_mp, radius, g_ref, w_ref, gain_ref, out_ref, gains_ref,
    part, recv, own, grad, sq_ref, stat, sums, gains,
    part_send, part_recv, hop_send, hop_recv, own_sem,
    stat_send, stat_recv, sums_send, sums_recv, gain_send, gain_recv,
):
    pos, core, hops, partner = ring(n)
    rows, half = part.shape[2], part.shape[3]
    sub = rows // SUBS
    total = n * SUBS
    tile = 16
    dp_peers, mp_peers = others("dp", 2 * n), others("mp", n_mp)
    greet([{axis: peer} for axis, peer in dp_peers + mp_peers])

    def block(t, d, which):
        s, i = t // SUBS, t % SUBS
        target = (pos + n - 1 - s + n) % n if d == 0 else (pos + 1 + s) % n
        start = (chip_at(target, n) * 2 + which) * rows + i * sub
        return g_ref.at[pl.ds(pl.multiple_of(start, tile), sub), pl.ds(d * half, half)]

    def piece(ref, t, d):
        return ref.at[t // SUBS, d, pl.ds(pl.multiple_of((t % SUBS) * sub, tile), sub)]

    def push(t, d):
        at = t * 2 + d
        return remote(
            block(t, d, 1 - core), piece(part, t, d), part_send.at[at], part_recv.at[at], partner
        )

    def load(t, d):
        return pltpu.make_async_copy(block(t, d, core), own.at[t % 2, d], own_sem.at[(t % 2) * 2 + d])

    def hop(t, d, src):
        at = t * 2 + d
        return remote(piece(src, t, d), piece(recv, t, d), hop_send.at[at], hop_recv.at[at], hops[d])

    for d in range(2):
        load(0, d).start()

    @pl.loop(0, SUBS)
    def _(t):
        for d in range(2):
            push(t, d).start()

    place = lax.axis_index("mp")
    fetch = pltpu.make_async_copy(w_ref, out_ref, own_sem.at[4])
    fetch.start()
    gain_copies = [
        remote(gain_ref, gains.at[place], gain_send.at[k], gain_recv.at[k], peer, axis)
        for k, (axis, peer) in enumerate(mp_peers)
    ]
    for copy in gain_copies:
        copy.start()
    gains[place] = gain_ref[...]
    sq_ref[...] = jnp.zeros_like(sq_ref)

    def step(t, first, last):
        @pl.when(t + 1 < total)
        def _():
            for d in range(2):
                load(t + 1, d).start()

        @pl.when(t + SUBS < total)
        def _():
            for d in range(2):
                push(t + SUBS, d).start()

        for d in range(2):
            load(t, d).wait()
            push(t, d).wait_recv()
            if not first:
                hop(t - SUBS, d, recv).wait_recv()
            source = piece(part, t, d)
            came = None if first else piece(recv, t - SUBS, d)
            mine = own.at[t % 2, d]

            @pl.loop(0, sub // tile)
            def _(r):
                at = pl.ds(pl.multiple_of(r * tile, tile), tile)
                value = mine[at, :].astype(jnp.float32) + source[at, :].astype(jnp.float32)
                if not first:
                    value = value + came[at, :].astype(jnp.float32)
                if last:
                    row = pl.multiple_of((t % SUBS) * sub + r * tile, tile)
                    grad[pl.ds(row, tile), d * half : (d + 1) * half] = value
                    squared = value * value
                    sq_ref[...] += squared[:8] + squared[8:]
                elif first:
                    source[at, :] = value.astype(jnp.bfloat16)
                else:
                    came[at, :] = value.astype(jnp.bfloat16)

        if not last:
            for d in range(2):
                at = t * 2 + d
                src = piece(part, t, d) if first else piece(recv, t - SUBS, d)
                remote(src, piece(recv, t, d), hop_send.at[at], hop_recv.at[at], hops[d]).start()

    @pl.loop(0, SUBS)
    def _(t):
        step(t, True, False)

    @pl.loop(SUBS, total - SUBS)
    def _(t):
        step(t, False, False)

    @pl.loop(total - SUBS, total)
    def _(t):
        step(t, False, True)

    folded = sq_ref[:, :128]
    for c in range(1, half // 128):
        folded = folded + sq_ref[:, c * 128 : (c + 1) * 128]
    stat[0] = folded

    @pl.loop(0, total)
    def _(t):
        for d in range(2):
            push(t, d).wait_send()

    @pl.loop(0, total - SUBS)
    def _(t):
        for d in range(2):
            hop(t, d, recv).wait_send()

    def share(slots, peers, send, arrive):
        copies = [
            remote(slots.at[0], slots.at[k + 1], send.at[k], arrive.at[k], peer, axis)
            for k, (axis, peer) in enumerate(peers)
        ]
        for copy in copies:
            copy.start()
        for copy in copies:
            copy.wait()
        return jnp.sum(slots[...], axis=0)

    sums[0] = share(stat, dp_peers, stat_send, stat_recv)
    for copy in gain_copies:
        copy.wait()
    gains_ref[...] = gains[...]
    fetch.wait()
    every = share(sums, mp_peers, sums_send, sums_recv)
    squares = jnp.sum(jnp.sum(every, axis=0, keepdims=True), axis=1, keepdims=True)
    scale = radius / jnp.sqrt(squares + 1e-12)

    @pl.loop(0, rows // tile)
    def _(r):
        at = pl.ds(pl.multiple_of(r * tile, tile), tile)
        value = out_ref[at, :].astype(jnp.float32) + scale * grad[at, :]
        out_ref[at, :] = value.astype(jnp.bfloat16)


def reduce_rows(n, n_mp, radius, grads, weights, gain):
    depth, cols = grads.shape
    rows, half = depth // (2 * n), cols // 2
    sub = rows // SUBS
    dma = pltpu.SemaphoreType.DMA
    return pl.pallas_call(
        functools.partial(scatter_kernel, n, n_mp, radius),
        out_shape=(
            jax.ShapeDtypeStruct((rows, cols), jnp.bfloat16),
            jax.ShapeDtypeStruct((n_mp, *gain.shape), jnp.float32),
        ),
        in_specs=[
            pl.BlockSpec(memory_space=pl.ANY),
            pl.BlockSpec(memory_space=pl.ANY),
            pl.BlockSpec(memory_space=pltpu.VMEM),
        ],
        out_specs=(
            pl.BlockSpec(memory_space=pltpu.VMEM),
            pl.BlockSpec(memory_space=pltpu.VMEM),
        ),
        scratch_shapes=[
            pltpu.VMEM((n, 2, rows, half), jnp.bfloat16),
            pltpu.VMEM((n - 1, 2, rows, half), jnp.bfloat16),
            pltpu.VMEM((2, 2, sub, half), jnp.bfloat16),
            pltpu.VMEM((rows, cols), jnp.float32),
            pltpu.VMEM((8, half), jnp.float32),
            pltpu.VMEM((2 * n, 8, 128), jnp.float32),
            pltpu.VMEM((n_mp, 8, 128), jnp.float32),
            pltpu.VMEM((n_mp, *gain.shape), jnp.float32),
            dma((n * SUBS * 2,)),
            dma((n * SUBS * 2,)),
            dma(((n - 1) * SUBS * 2,)),
            dma(((n - 1) * SUBS * 2,)),
            dma((5,)),
            dma((2 * n - 1,)),
            dma((2 * n - 1,)),
            dma((n_mp - 1,)),
            dma((n_mp - 1,)),
            dma((n_mp - 1,)),
            dma((n_mp - 1,)),
        ],
        compiler_params=pltpu.CompilerParams(
            collective_id=1, has_side_effects=True, vmem_limit_bytes=VMEM_LIMIT
        ),
        cost_estimate=pl.CostEstimate(
            flops=200 * 10**9, bytes_accessed=3 * grads.size, transcendentals=0
        ),
        name="reduce_rows",
    )(grads, weights, gain)


def gather_kernel(
    n, x_ref, gain_ref, p_ref, out_ref, normed, buf, pre_ref,
    hop_send, hop_recv, part_send, part_recv, own_sem, x_sem,
):
    pos, core, hops, partner = ring(n)
    rows, width = buf.shape[3] // 2, buf.shape[4]
    half = SUBS * width
    greet([{"dp": peer} for peer in (*hops, partner)])

    def mine(i, d):
        return p_ref.at[:, pl.ds(pl.multiple_of(d * half + i * width, 128), width)]

    def piece(s, i, d, which):
        return buf.at[s, d, i, pl.ds(pl.multiple_of(which * rows, 16), rows)]

    def hop(s, i, d, src):
        at = ((s - 1) * SUBS + i) * 2 + d
        return remote(src, piece(s, i, d, core), hop_send.at[at], hop_recv.at[at], hops[d])

    def push(s, i, d, src):
        at = (s * SUBS + i) * 2 + d
        return remote(src, piece(s, i, d, core), part_send.at[at], part_recv.at[at], partner)

    def pushed(s, i, d):
        at = (s * SUBS + i) * 2 + d
        there = piece(s, i, d, 1 - core)
        return remote(there, there, part_send.at[at], part_recv.at[at], partner)

    def keep(i, d):
        return pltpu.make_async_copy(mine(i, d), piece(0, i, d, core), own_sem.at[i * 2 + d])

    fetch = pltpu.make_async_copy(x_ref, normed, x_sem.at[0])
    fetch.start()
    for i in range(AHEAD):
        for d in range(2):
            hop(1, i, d, mine(i, d)).start()

    @pl.loop(0, SUBS)
    def _(i):
        for d in range(2):
            keep(i, d).start()
            push(0, i, d, mine(i, d)).start()

    pre_ref[...] = jnp.zeros_like(pre_ref)
    fetch.wait()

    @pl.loop(0, normed.shape[0] // 16)
    def _(r):
        at = pl.ds(pl.multiple_of(r * 16, 16), 16)
        values = normed[at, :].astype(jnp.float32)
        center = jnp.mean(values, axis=1, keepdims=True)
        moved = values - center
        spread = jnp.mean(moved * moved, axis=1, keepdims=True)
        scaled = moved * (1.0 / jnp.sqrt(spread + 1e-06)) * gain_ref[...]
        normed[at, :] = scaled.astype(jnp.bfloat16)

    def multiply(s, i):
        for d in range(2):
            pushed(s, i, d).wait_recv()
            owner = (pos + n - s) % n if d == 0 else (pos + s) % n
            cols = pl.ds(pl.multiple_of(chip_at(owner, n) * 2 * rows, 128), 2 * rows)
            out = pl.ds(pl.multiple_of(d * half + i * width, 128), width)
            pre_ref[:, out] += jnp.dot(
                normed[:, cols], buf[s, d, i], preferred_element_type=jnp.float32
            )

    def activate(i):
        tall = 64
        for d in range(2):
            cols = pl.ds(pl.multiple_of(d * half + i * width, 128), width)

            @pl.loop(0, pre_ref.shape[0] // tall)
            def _(r):
                at = pl.ds(pl.multiple_of(r * tall, tall), tall)
                pre = pre_ref[at, cols]
                value = 0.5 * pre * (1.0 + lax.erf(pre * math.sqrt(0.5)))
                out_ref[at, cols] = value.astype(jnp.bfloat16)

    @pl.loop(0, SUBS + n - 1)
    def _(wave):
        @pl.when(wave + AHEAD < SUBS)
        def _():
            for d in range(2):
                hop(1, wave + AHEAD, d, mine(wave + AHEAD, d)).start()

        for s in range(1, n):
            i = wave - (s - 1)

            @pl.when((i >= 0) & (i < SUBS))
            def _():
                for d in range(2):
                    hop(s, i, d, piece(s, i, d, core)).wait_recv()
                    if s < n - 1:
                        hop(s + 1, i, d, piece(s, i, d, core)).start()
                    push(s, i, d, piece(s, i, d, core)).start()

            if s == 1:

                @pl.when(wave < SUBS)
                def _():
                    for d in range(2):
                        keep(wave, d).wait()
                    multiply(0, wave)

            @pl.when((i >= 1) & (i <= SUBS))
            def _():
                multiply(s, i - 1)
                if s == n - 1:
                    activate(i - 1)

    @pl.loop(0, SUBS)
    def _(i):
        for d in range(2):
            for s in range(n):
                push(s, i, d, piece(s, i, d, core)).wait_send()
            for s in range(1, n):
                hop(s, i, d, piece(s, i, d, core)).wait_send()


def gather_matmul(n, feats, gains, perturbed):
    tokens, depth = feats.shape
    rows, cols = perturbed.shape
    half = cols // 2
    dma = pltpu.SemaphoreType.DMA
    return pl.pallas_call(
        functools.partial(gather_kernel, n),
        out_shape=jax.ShapeDtypeStruct((tokens, cols), jnp.bfloat16),
        in_specs=[
            pl.BlockSpec(memory_space=pl.ANY),
            pl.BlockSpec(memory_space=pltpu.VMEM),
            pl.BlockSpec(memory_space=pl.ANY),
        ],
        out_specs=pl.BlockSpec(memory_space=pltpu.VMEM),
        scratch_shapes=[
            pltpu.VMEM((tokens, depth), jnp.bfloat16),
            pltpu.VMEM((n, 2, SUBS, 2 * rows, half // SUBS), jnp.bfloat16),
            pltpu.VMEM((tokens, cols), jnp.float32),
            dma(((n - 1) * SUBS * 2,)),
            dma(((n - 1) * SUBS * 2,)),
            dma((n * SUBS * 2,)),
            dma((n * SUBS * 2,)),
            dma((SUBS * 2,)),
            dma((1,)),
        ],
        compiler_params=pltpu.CompilerParams(
            collective_id=2, has_side_effects=True, vmem_limit_bytes=VMEM_LIMIT
        ),
        cost_estimate=pl.CostEstimate(
            flops=2 * tokens * depth * cols,
            bytes_accessed=2 * depth * cols,
            transcendentals=0,
        ),
        name="gather_matmul",
    )(feats, gains, perturbed)


def ring_program(n, n_mp, radius, tokens, ln_gain, weights, grad_partials):
    feats = lax.all_gather(tokens, "mp", axis=1, tiled=True)
    gain = jnp.broadcast_to(ln_gain.astype(jnp.float32), (8, ln_gain.shape[0]))
    perturbed, gains = reduce_rows(n, n_mp, radius, grad_partials[0], weights, gain)
    hidden = gather_matmul(n, feats, gains[:, 0].reshape(1, -1), perturbed)
    return (hidden, perturbed)


def grid_kernel(
    n_mp, radius, x_ref, gain_ref, g_ref, w_ref, hid, wnew,
    part0, part1, recv0, recv1, own0, own1, grad, sq0, sq1, near, far,
    turned, zstat, stat, lead, landed,
    push_send, push_recv, hop_send, hop_recv, own_sem, load_sem,
    z_send, z_recv, stat_send, stat_recv,
    cross_send, cross_recv, relay_send, relay_recv, spread_send, spread_recv,
    y_send, y_recv, mine_send, mine_recv, pass_send, pass_recv, c_send, c_recv,
    head_send, head_recv,
):
    part, recv, own, sq = (part0, part1), (recv0, recv1), (own0, own1), (sq0, sq1)
    me, z = lax.axis_index("dp"), lax.axis_index("mp")
    core, x, y = me % 2, (me // 2) % 2, me // 4
    rows, width = part0.shape[1], (part0.shape[2], part1.shape[2])
    start_col = (0, width[0])
    sub, tile, tokens, feats = rows // SUBS, 16, hid.shape[0], near.shape[2]
    chunks = (width[0] // CHUNK, width[1] // CHUNK)

    def device(flip_x, flip_y, which):
        cx = 1 - x if flip_x else x
        cy = 1 - y if flip_y else y
        return (cy * 2 + cx) * 2 + which

    partner, x_peer, y_peer = device(0, 0, 1 - core), device(1, 0, core), device(0, 1, core)
    flips = (((1, 1), (1, 0), (0, 1), (0, 0)), ((1, 1), (0, 1), (1, 0), (0, 0)))
    hops = ((x_peer, x_peer, y_peer), (y_peer, y_peer, x_peer))
    everyone = [
        {"dp": (me + a) % 8, "mp": (z + b) % n_mp} for a in range(8) for b in range(n_mp) if a + b
    ]

    mine, ours = 2 * y + core, 2 * y + 1 - core
    theirs, others_there = 2 * (1 - y) + core, 2 * (1 - y) + 1 - core

    def span(i, size):
        return pl.ds(pl.multiple_of(i * size, size), size)

    def block(s, i, d, which):
        start = device(*flips[d][s], which) * rows + i * sub
        return g_ref.at[pl.ds(pl.multiple_of(start, tile), sub), pl.ds(start_col[d], width[d])]

    def piece(ref, s, i):
        return ref.at[s, span(i, sub)]

    def push(s, i, d):
        at = (s * SUBS + i) * 2 + d
        return remote(
            block(s, i, d, 1 - core), piece(part[d], s, i), push_send.at[d], push_recv.at[at], partner
        )

    def load(s, i, d, slot):
        return pltpu.make_async_copy(block(s, i, d, core), own[d].at[slot], own_sem.at[slot * 2 + d])

    def hop(s, i, d):
        at = (s * SUBS + i) * 2 + d
        return remote(
            piece(part[d], s, i), piece(recv[d], s, i), hop_send.at[d], hop_recv.at[at], hops[d][s]
        )

    def add(s, i, slot):
        for d in range(2):
            load(s, i, d, slot).wait()
            push(s, i, d).wait_recv()
            came = {0: (), 1: (), 2: (0,), 3: (1, 2)}[s]
            if s > 1:
                hop(2 * s - 4, i, d).wait_recv()
            source, mine = piece(part[d], s, i), own[d].at[slot]
            extra = [piece(recv[d], k, i) for k in came]

            @pl.loop(0, sub // tile)
            def _(r):
                at = span(r, tile)
                value = mine[at, :].astype(jnp.float32) + source[at, :].astype(jnp.float32)
                for ref in extra:
                    value = value + ref[at, :].astype(jnp.float32)
                if s == 3:
                    row = pl.multiple_of(i * sub + r * tile, tile)
                    grad[pl.ds(row, tile), start_col[d] : start_col[d] + width[d]] = value
                    squared = value * value
                    sq[d][...] += squared[:8] + squared[8:]
                else:
                    source[at, :] = value.astype(jnp.bfloat16)

            if s < 3:
                hop(s, i, d).start()

    def both(make, *args):
        for d in range(2):
            make(*args[:2], d, *args[2:]).start()

    fetch = pltpu.make_async_copy(x_ref, hid.at[:, pl.ds(0, feats)], load_sem.at[0])
    fetch_w = pltpu.make_async_copy(w_ref, wnew, load_sem.at[1])
    tall, lines = turned.shape[1], 64

    def z_copy(k):
        return remote(
            zstat.at[z], zstat.at[z], z_send.at[k], z_recv.at[k], (z + k + 1) % n_mp, "mp"
        )

    def gather_statistics():
        fetch.wait()

        @pl.loop(0, tokens // tall)
        def _(b):
            @pl.loop(0, tall // lines)
            def _(r):
                at = pl.ds(pl.multiple_of(b * tall + r * lines, lines), lines)
                values = hid[at, :feats].astype(jnp.float32)
                center = jnp.mean(values, axis=1, keepdims=True)
                moved = values - center
                spread = jnp.sum(moved * moved, axis=1, keepdims=True)
                turned[0, span(r, lines), :] = jnp.broadcast_to(center, (lines, tall))
                turned[1, span(r, lines), :] = jnp.broadcast_to(spread, (lines, tall))

            for k in range(2):
                zstat[z, k, b] = turned[k].T[:8]

        for k in range(n_mp - 1):
            z_copy(k).start()

    belongs = (z + x) % 2 == 0
    half = tokens // 2

    def cross_copy(send):
        src = hid.at[pl.ds(0, half), pl.ds(0, feats)] if send == 0 else relay_room
        return remote(
            src, far.at[z // 2, pl.ds(send * half, half)], cross_send.at[0], cross_recv.at[0], x_peer
        )

    relay_room = hid.at[pl.ds(0, half), pl.ds(feats, feats)]
    relay_copy = remote(
        hid.at[pl.ds(half, half), pl.ds(0, feats)], relay_room,
        relay_send.at[0], relay_recv.at[0], z + 1 - 2 * (z % 2), "mp",
    )

    ends = ((3 * x, x), (2 - x, 1 - x))
    items = [(o, near.at[k, pl.ds(h * half, half)]) for o, k in ends for h in range(2)]
    items += [(x + 2 * k, far.at[k, pl.ds(0, half)]) for k in range(2)]
    items += [(1 - x + 2 * k, far.at[k, pl.ds(half, half)]) for k in range(2)]
    near_top, long_low, short_low, far_top, far_low = (0, 2), (1,), (3,), (4, 5), (6, 7)

    def spread_copy(k, way):
        return remote(
            items[k][1], items[k][1], spread_send.at[k * 2 + way], spread_recv.at[k],
            z + 1 - 2 * way, "mp",
        )

    def spread(which, steps):
        for k in which:
            away = z - items[k][0]
            if steps == 0 and k >= 4:

                @pl.when(away == 0)
                def _():
                    cross_copy(0).wait_recv()

            for way, sign in ((0, 1), (1, -1)):
                @pl.when((away * sign == steps) & ((z < n_mp - 1) if way == 0 else (z > 0)))
                def _():
                    if steps > 0:
                        spread_copy(k, way).wait_recv()
                    spread_copy(k, way).start()

    def spread_arrived(which):
        for k in which:
            away = z - items[k][0]

            @pl.when(((z == 0) & (away < 0)) | ((z == n_mp - 1) & (away > 0)))
            def _():
                spread_copy(k, 0).wait_recv()

    def spread_sent():
        for k in range(8):
            away = z - items[k][0]

            @pl.when((away >= 0) & (z < n_mp - 1))
            def _():
                spread_copy(k, 0).wait_send()

            @pl.when((away <= 0) & (z > 0))
            def _():
                spread_copy(k, 1).wait_send()

        cross_copy(0).wait_send()

        @pl.when((z + x) % 2 == 1)
        def _():
            relay_copy.wait_send()

    def normalise():
        for k in range(n_mp - 1):
            z_copy(k).wait_recv()
        centers = [zstat[k, 0] for k in range(n_mp)]
        center = sum(centers) * (1.0 / n_mp)
        squared = sum(zstat[k, 1] for k in range(n_mp))
        squared = squared + feats * sum((one - center) * (one - center) for one in centers)
        scaled = 1.0 / jnp.sqrt(squared * (1.0 / (feats * n_mp)) + 1e-06)
        for k in range(n_mp - 1):
            z_copy(k).wait_send()
        zstat[0, 0] = center
        zstat[0, 1] = scaled

        for h in range(2):
            @pl.loop(h * half // tall, (h + 1) * half // tall)
            def _(b):
                for k in range(2):
                    turned[k] = jnp.broadcast_to(zstat[0, k, b][:1], (tall, tall)).T

                @pl.loop(0, tall // lines)
                def _(r):
                    at = pl.ds(pl.multiple_of(b * tall + r * lines, lines), lines)
                    values = hid[at, :feats].astype(jnp.float32)
                    moved = values - turned[0, span(r, lines), :1]
                    value = moved * turned[1, span(r, lines), :1] * gain_ref[...].astype(jnp.float32).reshape(1, feats)
                    value = value.astype(jnp.bfloat16)
                    hid[at, :feats] = value

                    @pl.when(belongs)
                    def _():
                        near[z // 2, at, :] = value

            @pl.when((z + x) % 2 == 1)
            def _():
                (cross_copy(0) if h == 0 else relay_copy).start()

            spread(near_top if h == 0 else long_low + short_low, 0)

    def relay():
        @pl.when(belongs)
        def _():
            relay_copy.wait_recv()
            cross_copy(1).start()

    def events(i, table):
        for k, actions in table.items():
            @pl.when(i == k)
            def _():
                for action in actions:
                    action()

    def later(which, steps):
        return lambda: spread(which, steps)

    fetch.start()
    both(load, 0, 0, 0)
    sq0[...] = jnp.zeros_like(sq0)
    sq1[...] = jnp.zeros_like(sq1)
    greet(everyone)

    @pl.loop(0, SUBS)
    def _(i):
        both(push, 0, i)

    @pl.loop(0, SUBS)
    def _(i):
        @pl.when(i + 1 < SUBS)
        def _():
            both(load, 0, i + 1, (i + 1) % 2)

        @pl.when(i + 1 == SUBS)
        def _():
            both(load, 1, 0, 0)

        both(push, 1, i)
        both(push, 2, i)
        add(0, i, i % 2)
        events(i, {0: [gather_statistics], 2: [normalise]})

    @pl.loop(0, SUBS)
    def _(i):
        both(load, 2, i, 1)
        both(push, 3, i)
        add(1, i, 0)

        @pl.when(i + 1 < SUBS)
        def _():
            both(load, 1, i + 1, 0)

        @pl.when(i + 1 == SUBS)
        def _():
            both(load, 3, 0, 0)

        add(2, i, 1)
        events(
            i,
            {
                0: [relay],
                2: [later(near_top, 1)],
                3: [later(far_top, 0)],
                4: [later(short_low, 1)],
            },
        )

    fetch_w.start()

    @pl.loop(0, SUBS)
    def _(i):
        @pl.when(i + 1 < SUBS)
        def _():
            both(load, 3, i + 1, (i + 1) % 2)

        for d in range(2):
            hop(1, i, d).wait_recv()
        events(
            i,
            {
                0: [later(near_top, 2), later(far_low, 0)],
                3: [later(far_top, 2), later(far_low, 2)],
            },
        )
        add(3, i, i % 2)
        events(i, {0: [later(far_top, 1)], 1: [later(far_low, 1)], 2: [later(long_low, 1)]})

    folded = jnp.zeros((8, 128), jnp.float32)
    for d in range(2):
        for c in range(width[d] // 128):
            folded = folded + sq[d][:, c * 128 : (c + 1) * 128]
    stat[0] = folded

    for d in range(2):
        remote(part[d], part[d], push_send.at[d], push_recv.at[0], partner).wait_send()
        sent = part[d].at[pl.ds(0, 3)]
        remote(sent, recv[d], hop_send.at[d], hop_recv.at[0], partner).wait_send()

    def shared(src, dst, device_id):
        return pltpu.make_async_remote_copy(
            src_ref=src,
            dst_ref=dst,
            send_sem=stat_send.at[0],
            recv_sem=stat_recv.at[0],
            device_id=device_id,
            device_id_type=pl.DeviceIdType.MESH,
        )

    for k, device_id in enumerate(everyone):
        shared(stat.at[pl.ds(0, 1)], stat.at[pl.ds(k + 1, 1)], device_id).start()
    fetch_w.wait()

    top = rows // 2

    def head(k):
        here = part0.at[mine, pl.ds(top, top), pl.ds(0, CHUNK)]
        src = (wnew.at[pl.ds(0, top), pl.ds(0, CHUNK)], lead, here)[k]
        dst = (landed.at[0], landed.at[1], here)[k]
        return remote(src, dst, head_send.at[k], head_recv.at[k], y_peer)

    head(0).start()
    lead[...] = grad[:top, :CHUNK].astype(jnp.bfloat16)
    head(1).start()
    rest = stat.at[pl.ds(1, len(everyone))]
    shared(rest, rest, everyone[0]).wait()
    every = jnp.sum(stat[...], axis=0)
    squares = jnp.sum(jnp.sum(every, axis=0, keepdims=True), axis=1, keepdims=True)
    scale = radius / jnp.sqrt(squares + 1e-12)


    def slab(d, slot, j):
        return part[d].at[slot, :, span(j, CHUNK)]

    def across(d, j):
        at = d * chunks[0] + j
        here = slab(d, mine, j)
        return remote(here, here, y_send.at[d], y_recv.at[at], y_peer)

    def across_arrived(d, j):
        at = d * chunks[0] + j
        here = slab(d, theirs, j)
        return remote(here, here, y_send.at[d], y_recv.at[at], y_peer)

    def give(d, j, slot):
        at = d * chunks[0] + j
        here = slab(d, mine if slot == "mine" else theirs, j)
        sems = (mine_send, mine_recv) if slot == "mine" else (pass_send, pass_recv)
        return remote(here, here, sems[0].at[d], sems[1].at[at], partner)

    def given(d, j, slot):
        at = d * chunks[0] + j
        here = slab(d, ours if slot == "mine" else others_there, j)
        sems = (mine_send, mine_recv) if slot == "mine" else (pass_send, pass_recv)
        return remote(here, here, sems[0].at[d], sems[1].at[at], partner)

    def partial_copy(d, j):
        at = d * chunks[0] + j
        return remote(
            recv[d].at[0, :, span(j, CHUNK)], recv[d].at[1, :, span(j, CHUNK)],
            c_send.at[d], c_recv.at[at], x_peer,
        )

    def columns(d, j):
        return pl.ds(pl.multiple_of(start_col[d] + j * CHUNK, 128), CHUNK)

    def perturb(d, j):
        cols = columns(d, j)

        @pl.loop(0, rows // 256)
        def _(r):
            at = span(r, 256)
            value = wnew[at, cols].astype(jnp.float32) + scale * grad[at, cols]
            value = value.astype(jnp.bfloat16)
            wnew[at, cols] = value
            part[d][mine, at, span(j, CHUNK)] = value

    for k in range(2):
        head(k).wait_send()
    perturb(0, 0)
    head(2).start()
    give(0, 0, "mine").start()
    for d in range(2):
        @pl.loop(1 - d, chunks[d])
        def _(j):
            perturb(d, j)
            across(d, j).start()

    def give_next(d, j):
        @pl.when(j + 1 < chunks[d])
        def _():
            give(d, j + 1, "mine").start()

        if d == 0:

            @pl.when(j + 1 == chunks[0])
            def _():
                give(1, 0, "mine").start()

    def arrive_first():
        for k in range(2):
            head(k).wait_recv()
        value = landed[0].astype(jnp.float32) + scale * landed[1].astype(jnp.float32)
        part0[theirs, :top, :CHUNK] = value.astype(jnp.bfloat16)
        there = part0.at[theirs, pl.ds(top, top), pl.ds(0, CHUNK)]
        remote(there, there, head_send.at[2], head_recv.at[2], y_peer).wait_recv()
        give(0, 0, "theirs").start()
        give_next(0, 0)

    def product(left, at, d, j, size):
        total = None
        for k in range(2):
            right = part[d][2 * k : 2 * k + 2, :, span(j, size)].reshape(2 * rows, size)
            one = jnp.dot(left[k, at], right, preferred_element_type=jnp.float32)
            total = one if total is None else total + one
        return total

    def arrive(d, j):
        across_arrived(d, j).wait_recv()
        give(d, j, "theirs").start()
        give_next(d, j)

    def send_far(d, j):
        given(d, j, "mine").wait_recv()
        given(d, j, "theirs").wait_recv()
        recv[d][0, :, span(j, CHUNK)] = product(far, pl.ds(0, tokens), d, j, CHUNK).astype(jnp.bfloat16)
        partial_copy(d, j).start()

    def keep_near(d, g, h):
        size, at = GROUP * CHUNK, pl.ds(h * half, half)
        cols = pl.ds(pl.multiple_of(start_col[d] + g * size, 128), size)
        grad[at, cols] = product(near, at, d, g, size)

    def settle(d):
        here, there, partial = part[d].at[mine], part[d].at[theirs], recv[d].at[0]
        first = CHUNK * (1 - d)
        sent = part[d].at[mine, :, pl.ds(first, width[d] - first)]
        remote(sent, sent, y_send.at[d], y_recv.at[0], y_peer).wait_send()
        remote(here, here, mine_send.at[d], mine_recv.at[0], partner).wait_send()
        remote(there, there, pass_send.at[d], pass_recv.at[0], partner).wait_send()
        remote(partial, partial, c_send.at[d], c_recv.at[0], x_peer).wait_send()

    def finish(d, j):
        cols = columns(d, j)
        partial_copy(d, j).wait_recv()

        @pl.loop(0, tokens // 64)
        def _(r):
            at = span(r, 64)
            pre = grad[at, cols] + recv[d][1, at, span(j, CHUNK)].astype(jnp.float32)
            value = 0.5 * pre * (1.0 + lax.erf(pre * math.sqrt(0.5)))
            hid[at, cols] = value.astype(jnp.bfloat16)

    spread(long_low, 2)
    spread_arrived(far_top + far_low)

    arrive_first()
    send_far(0, 0)

    @pl.loop(1, chunks[0])
    def _(j):
        arrive(0, j)
        send_far(0, j)

    spread_arrived(near_top + long_low + short_low)
    groups = (chunks[0] // GROUP, chunks[1] // GROUP)
    turns = [0, 1] + [1 + GROUP * k for k in range(1, 2 * groups[0] - 1)]
    spread_sent()

    @pl.loop(0, chunks[1])
    def _(j):
        arrive(1, j)

        @pl.when(j > GROUP)
        def _():
            finish(1, j - GROUP - 1)

        for g in range(groups[0]):
            for k in range(GROUP):
                @pl.when(j == turns[2 * g + 1] + 1 + k)
                def _():
                    finish(0, g * GROUP + k)

        send_far(1, j)

        @pl.when(j % GROUP == GROUP - 1)
        def _():
            keep_near(1, j // GROUP, 0)

        @pl.when((j % GROUP == 0) & (j > 0))
        def _():
            keep_near(1, j // GROUP - 1, 1)

        for k, turn in enumerate(turns):
            @pl.when(j == turn)
            def _():
                keep_near(0, k // 2, k % 2)

    keep_near(1, groups[1] - 1, 1)
    for j in range(max(chunks[1] - turns[-1] - 1, 0), GROUP):
        finish(0, chunks[0] - GROUP + j)
    for j in range(chunks[1] - GROUP - 1, chunks[1]):
        finish(1, j)

    head(2).wait_send()
    for d in range(2):
        settle(d)


def store_kernel(hid, weights, hid_out, w_out, sem):
    strip = hid.shape[0] // STRIPS
    copies = []
    for k, (src, dst) in enumerate(((hid, hid_out), (weights, w_out))):
        for i in range(STRIPS):
            at = pl.ds(i * strip, strip)
            copies.append(pltpu.make_async_copy(src.at[at], dst.at[at], sem.at[k * STRIPS + i]))
    for copy in copies:
        copy.start()
    for copy in copies:
        copy.wait()


def store(hid, weights):
    anywhere, inside = pl.BlockSpec(memory_space=pl.ANY), pl.BlockSpec(memory_space=pltpu.VMEM)
    hid = pltpu.with_memory_space_constraint(hid, pltpu.VMEM)
    weights = pltpu.with_memory_space_constraint(weights, pltpu.VMEM)
    return pl.pallas_call(
        store_kernel,
        out_shape=(
            jax.ShapeDtypeStruct(hid.shape, hid.dtype),
            jax.ShapeDtypeStruct(weights.shape, weights.dtype),
        ),
        in_specs=[inside, inside],
        out_specs=(anywhere, anywhere),
        scratch_shapes=[pltpu.SemaphoreType.DMA((2 * STRIPS,))],
        compiler_params=pltpu.CompilerParams(vmem_limit_bytes=1000000),
        name="store",
    )(hid, weights)


def grid_program(n_mp, radius, tokens, gain, weights, grads):
    depth, cols = grads.shape
    rows = depth // 8
    count, feats = tokens.shape
    unit = GROUP * CHUNK
    first = cols * 3 // 8 // unit * unit
    wide = (first, cols - first)
    sub, pieces = rows // SUBS, cols // CHUNK
    dma = pltpu.SemaphoreType.DMA
    bf16, f32 = jnp.bfloat16, jnp.float32
    anywhere = pl.BlockSpec(memory_space=pl.ANY)
    return pl.pallas_call(
        functools.partial(grid_kernel, n_mp, radius),
        out_shape=(
            pltpu.VMEM((count, cols), bf16),
            pltpu.VMEM((rows, cols), bf16),
        ),
        in_specs=[anywhere, pl.BlockSpec(memory_space=pltpu.VMEM), anywhere, anywhere],
        out_specs=(pl.BlockSpec(memory_space=pltpu.VMEM), pl.BlockSpec(memory_space=pltpu.VMEM)),
        scratch_shapes=[
            pltpu.VMEM((4, rows, wide[0]), bf16),
            pltpu.VMEM((4, rows, wide[1]), bf16),
            pltpu.VMEM((3, rows, wide[0]), bf16),
            pltpu.VMEM((3, rows, wide[1]), bf16),
            pltpu.VMEM((2, sub, wide[0]), bf16),
            pltpu.VMEM((2, sub, wide[1]), bf16),
            pltpu.VMEM((rows, cols), f32),
            pltpu.VMEM((8, wide[0]), f32),
            pltpu.VMEM((8, wide[1]), f32),
            pltpu.VMEM((2, count, feats), bf16),
            pltpu.VMEM((2, count, feats), bf16),
            pltpu.VMEM((2, 128, 128), f32),
            pltpu.VMEM((n_mp, 2, count // 128, 8, 128), f32),
            pltpu.VMEM((8 * n_mp, 8, 128), f32),
            pltpu.VMEM((rows // 2, CHUNK), bf16),
            pltpu.VMEM((2, rows // 2, CHUNK), bf16),
            dma((2,)),
            dma((8 * SUBS,)),
            dma((2,)),
            dma((6 * SUBS,)),
            dma((4,)),
            dma((2,)),
            dma((n_mp - 1,)),
            dma((n_mp - 1,)),
            dma((1,)),
            dma((1,)),
            dma((1,)),
            dma((1,)),
            dma((1,)),
            dma((1,)),
            dma((16,)),
            dma((8,)),
        ]
        + [dma((2,)), dma((pieces,))] * 4
        + [dma((3,))] * 2,
        compiler_params=pltpu.CompilerParams(
            collective_id=3, has_side_effects=True, vmem_limit_bytes=57000000
        ),
        name="grid_program",
    )(tokens, gain, grads, weights)


def per_device(n, n_mp, width, tokens, ln_gain, weights, grad_partials):
    radius = 0.7 * math.sqrt(width)
    if n == 4 and n_mp == 4 and weights.shape[1] % (8 * GROUP * CHUNK) == 0:
        return store(*grid_program(n_mp, radius, tokens, ln_gain, weights, grad_partials[0]))
    return ring_program(n, n_mp, radius, tokens, ln_gain, weights, grad_partials)


def solution(mesh):
    placed = (P("dp", "mp"), P("mp"), P("dp", "mp"), P("dp", None, "mp"))

    def whole(tokens, ln_gain, weights, grad_partials):
        return jax.shard_map(
            functools.partial(per_device, mesh.shape["dp"] // 2, mesh.shape["mp"], weights.shape[1]),
            mesh=mesh,
            in_specs=placed,
            out_specs=(P("dp", "mp"), P("dp", "mp")),
            check_vma=False,
        )(tokens, ln_gain, weights, grad_partials)

    return whole
```

```python
import functools
import math

import jax
import jax.numpy as jnp
from jax import lax
from jax.experimental import pallas as pl
from jax.experimental.pallas import tpu as pltpu
from jax.sharding import PartitionSpec as P

SUBS = 6
AHEAD = 2
CHUNK = 128
GROUP = 3
STRIPS = 2
VMEM_LIMIT = 66 * 1000 * 1000


def power_of_two(n):
    return n & (n - 1) == 0


def chip_at(pos, n):
    if not power_of_two(n):
        return pos
    bits = n.bit_length() - 1
    out = 0
    for b in range(bits):
        out = out + ((pos // 2**b + pos // 2 ** (b + 1)) % 2) * 2**b
    return out


def position_of(chip, n):
    if not power_of_two(n):
        return chip
    bits = n.bit_length() - 1
    above, out = 0, 0
    for b in reversed(range(bits)):
        above = (chip // 2**b + above) % 2
        out = out + above * 2**b
    return out


def ring(n):
    me = lax.axis_index("dp")
    chip, core = me // 2, me % 2
    pos = position_of(chip, n)
    right = chip_at((pos + 1) % n, n) * 2 + core
    left = chip_at((pos + n - 1) % n, n) * 2 + core
    return pos, core, (right, left), chip * 2 + 1 - core


def greet(peers):
    barrier = pltpu.get_barrier_semaphore()
    for device_id in peers:
        pl.semaphore_signal(
            barrier, inc=1, device_id=device_id, device_id_type=pl.DeviceIdType.MESH
        )
    pl.semaphore_wait(barrier, len(peers))


def others(axis, size):
    me = lax.axis_index(axis)
    return [(axis, (me + k) % size) for k in range(1, size)]


def remote(src, dst, send, recv, peer, axis="dp"):
    return pltpu.make_async_remote_copy(
        src_ref=src,
        dst_ref=dst,
        send_sem=send,
        recv_sem=recv,
        device_id={axis: peer},
        device_id_type=pl.DeviceIdType.MESH,
    )


def scatter_kernel(
    n, n_mp, radius, g_ref, w_ref, gain_ref, out_ref, gains_ref,
    part, recv, own, grad, sq_ref, stat, sums, gains,
    part_send, part_recv, hop_send, hop_recv, own_sem,
    stat_send, stat_recv, sums_send, sums_recv, gain_send, gain_recv,
):
    pos, core, hops, partner = ring(n)
    rows, half = part.shape[2], part.shape[3]
    sub = rows // SUBS
    total = n * SUBS
    tile = 16
    dp_peers, mp_peers = others("dp", 2 * n), others("mp", n_mp)
    greet([{axis: peer} for axis, peer in dp_peers + mp_peers])

    def block(t, d, which):
        s, i = t // SUBS, t % SUBS
        target = (pos + n - 1 - s + n) % n if d == 0 else (pos + 1 + s) % n
        start = (chip_at(target, n) * 2 + which) * rows + i * sub
        return g_ref.at[pl.ds(pl.multiple_of(start, tile), sub), pl.ds(d * half, half)]

    def piece(ref, t, d):
        return ref.at[t // SUBS, d, pl.ds(pl.multiple_of((t % SUBS) * sub, tile), sub)]

    def push(t, d):
        at = t * 2 + d
        return remote(
            block(t, d, 1 - core), piece(part, t, d), part_send.at[at], part_recv.at[at], partner
        )

    def load(t, d):
        return pltpu.make_async_copy(block(t, d, core), own.at[t % 2, d], own_sem.at[(t % 2) * 2 + d])

    def hop(t, d, src):
        at = t * 2 + d
        return remote(piece(src, t, d), piece(recv, t, d), hop_send.at[at], hop_recv.at[at], hops[d])

    for d in range(2):
        load(0, d).start()

    @pl.loop(0, SUBS)
    def _(t):
        for d in range(2):
            push(t, d).start()

    place = lax.axis_index("mp")
    fetch = pltpu.make_async_copy(w_ref, out_ref, own_sem.at[4])
    fetch.start()
    gain_copies = [
        remote(gain_ref, gains.at[place], gain_send.at[k], gain_recv.at[k], peer, axis)
        for k, (axis, peer) in enumerate(mp_peers)
    ]
    for copy in gain_copies:
        copy.start()
    gains[place] = gain_ref[...]
    sq_ref[...] = jnp.zeros_like(sq_ref)

    def step(t, first, last):
        @pl.when(t + 1 < total)
        def _():
            for d in range(2):
                load(t + 1, d).start()

        @pl.when(t + SUBS < total)
        def _():
            for d in range(2):
                push(t + SUBS, d).start()

        for d in range(2):
            load(t, d).wait()
            push(t, d).wait_recv()
            if not first:
                hop(t - SUBS, d, recv).wait_recv()
            source = piece(part, t, d)
            came = None if first else piece(recv, t - SUBS, d)
            mine = own.at[t % 2, d]

            @pl.loop(0, sub // tile)
            def _(r):
                at = pl.ds(pl.multiple_of(r * tile, tile), tile)
                value = mine[at, :].astype(jnp.float32) + source[at, :].astype(jnp.float32)
                if not first:
                    value = value + came[at, :].astype(jnp.float32)
                if last:
                    row = pl.multiple_of((t % SUBS) * sub + r * tile, tile)
                    grad[pl.ds(row, tile), d * half : (d + 1) * half] = value
                    squared = value * value
                    sq_ref[...] += squared[:8] + squared[8:]
                elif first:
                    source[at, :] = value.astype(jnp.bfloat16)
                else:
                    came[at, :] = value.astype(jnp.bfloat16)

        if not last:
            for d in range(2):
                at = t * 2 + d
                src = piece(part, t, d) if first else piece(recv, t - SUBS, d)
                remote(src, piece(recv, t, d), hop_send.at[at], hop_recv.at[at], hops[d]).start()

    @pl.loop(0, SUBS)
    def _(t):
        step(t, True, False)

    @pl.loop(SUBS, total - SUBS)
    def _(t):
        step(t, False, False)

    @pl.loop(total - SUBS, total)
    def _(t):
        step(t, False, True)

    folded = sq_ref[:, :128]
    for c in range(1, half // 128):
        folded = folded + sq_ref[:, c * 128 : (c + 1) * 128]
    stat[0] = folded

    @pl.loop(0, total)
    def _(t):
        for d in range(2):
            push(t, d).wait_send()

    @pl.loop(0, total - SUBS)
    def _(t):
        for d in range(2):
            hop(t, d, recv).wait_send()

    def share(slots, peers, send, arrive):
        copies = [
            remote(slots.at[0], slots.at[k + 1], send.at[k], arrive.at[k], peer, axis)
            for k, (axis, peer) in enumerate(peers)
        ]
        for copy in copies:
            copy.start()
        for copy in copies:
            copy.wait()
        return jnp.sum(slots[...], axis=0)

    sums[0] = share(stat, dp_peers, stat_send, stat_recv)
    for copy in gain_copies:
        copy.wait()
    gains_ref[...] = gains[...]
    fetch.wait()
    every = share(sums, mp_peers, sums_send, sums_recv)
    squares = jnp.sum(jnp.sum(every, axis=0, keepdims=True), axis=1, keepdims=True)
    scale = radius / jnp.sqrt(squares + 1e-12)

    @pl.loop(0, rows // tile)
    def _(r):
        at = pl.ds(pl.multiple_of(r * tile, tile), tile)
        value = out_ref[at, :].astype(jnp.float32) + scale * grad[at, :]
        out_ref[at, :] = value.astype(jnp.bfloat16)


def reduce_rows(n, n_mp, radius, grads, weights, gain):
    depth, cols = grads.shape
    rows, half = depth // (2 * n), cols // 2
    sub = rows // SUBS
    dma = pltpu.SemaphoreType.DMA
    return pl.pallas_call(
        functools.partial(scatter_kernel, n, n_mp, radius),
        out_shape=(
            jax.ShapeDtypeStruct((rows, cols), jnp.bfloat16),
            jax.ShapeDtypeStruct((n_mp, *gain.shape), jnp.float32),
        ),
        in_specs=[
            pl.BlockSpec(memory_space=pl.ANY),
            pl.BlockSpec(memory_space=pl.ANY),
            pl.BlockSpec(memory_space=pltpu.VMEM),
        ],
        out_specs=(
            pl.BlockSpec(memory_space=pltpu.VMEM),
            pl.BlockSpec(memory_space=pltpu.VMEM),
        ),
        scratch_shapes=[
            pltpu.VMEM((n, 2, rows, half), jnp.bfloat16),
            pltpu.VMEM((n - 1, 2, rows, half), jnp.bfloat16),
            pltpu.VMEM((2, 2, sub, half), jnp.bfloat16),
            pltpu.VMEM((rows, cols), jnp.float32),
            pltpu.VMEM((8, half), jnp.float32),
            pltpu.VMEM((2 * n, 8, 128), jnp.float32),
            pltpu.VMEM((n_mp, 8, 128), jnp.float32),
            pltpu.VMEM((n_mp, *gain.shape), jnp.float32),
            dma((n * SUBS * 2,)),
            dma((n * SUBS * 2,)),
            dma(((n - 1) * SUBS * 2,)),
            dma(((n - 1) * SUBS * 2,)),
            dma((5,)),
            dma((2 * n - 1,)),
            dma((2 * n - 1,)),
            dma((n_mp - 1,)),
            dma((n_mp - 1,)),
            dma((n_mp - 1,)),
            dma((n_mp - 1,)),
        ],
        compiler_params=pltpu.CompilerParams(
            collective_id=1, has_side_effects=True, vmem_limit_bytes=VMEM_LIMIT
        ),
        cost_estimate=pl.CostEstimate(
            flops=200 * 10**9, bytes_accessed=3 * grads.size, transcendentals=0
        ),
        name="reduce_rows",
    )(grads, weights, gain)


def gather_kernel(
    n, x_ref, gain_ref, p_ref, out_ref, normed, buf, pre_ref,
    hop_send, hop_recv, part_send, part_recv, own_sem, x_sem,
):
    pos, core, hops, partner = ring(n)
    rows, width = buf.shape[3] // 2, buf.shape[4]
    half = SUBS * width
    greet([{"dp": peer} for peer in (*hops, partner)])

    def mine(i, d):
        return p_ref.at[:, pl.ds(pl.multiple_of(d * half + i * width, 128), width)]

    def piece(s, i, d, which):
        return buf.at[s, d, i, pl.ds(pl.multiple_of(which * rows, 16), rows)]

    def hop(s, i, d, src):
        at = ((s - 1) * SUBS + i) * 2 + d
        return remote(src, piece(s, i, d, core), hop_send.at[at], hop_recv.at[at], hops[d])

    def push(s, i, d, src):
        at = (s * SUBS + i) * 2 + d
        return remote(src, piece(s, i, d, core), part_send.at[at], part_recv.at[at], partner)

    def pushed(s, i, d):
        at = (s * SUBS + i) * 2 + d
        there = piece(s, i, d, 1 - core)
        return remote(there, there, part_send.at[at], part_recv.at[at], partner)

    def keep(i, d):
        return pltpu.make_async_copy(mine(i, d), piece(0, i, d, core), own_sem.at[i * 2 + d])

    fetch = pltpu.make_async_copy(x_ref, normed, x_sem.at[0])
    fetch.start()
    for i in range(AHEAD):
        for d in range(2):
            hop(1, i, d, mine(i, d)).start()

    @pl.loop(0, SUBS)
    def _(i):
        for d in range(2):
            keep(i, d).start()
            push(0, i, d, mine(i, d)).start()

    pre_ref[...] = jnp.zeros_like(pre_ref)
    fetch.wait()

    @pl.loop(0, normed.shape[0] // 16)
    def _(r):
        at = pl.ds(pl.multiple_of(r * 16, 16), 16)
        values = normed[at, :].astype(jnp.float32)
        center = jnp.mean(values, axis=1, keepdims=True)
        moved = values - center
        spread = jnp.mean(moved * moved, axis=1, keepdims=True)
        scaled = moved * (1.0 / jnp.sqrt(spread + 1e-06)) * gain_ref[...]
        normed[at, :] = scaled.astype(jnp.bfloat16)

    def multiply(s, i):
        for d in range(2):
            pushed(s, i, d).wait_recv()
            owner = (pos + n - s) % n if d == 0 else (pos + s) % n
            cols = pl.ds(pl.multiple_of(chip_at(owner, n) * 2 * rows, 128), 2 * rows)
            out = pl.ds(pl.multiple_of(d * half + i * width, 128), width)
            pre_ref[:, out] += jnp.dot(
                normed[:, cols], buf[s, d, i], preferred_element_type=jnp.float32
            )

    def activate(i):
        tall = 64
        for d in range(2):
            cols = pl.ds(pl.multiple_of(d * half + i * width, 128), width)

            @pl.loop(0, pre_ref.shape[0] // tall)
            def _(r):
                at = pl.ds(pl.multiple_of(r * tall, tall), tall)
                pre = pre_ref[at, cols]
                value = 0.5 * pre * (1.0 + lax.erf(pre * math.sqrt(0.5)))
                out_ref[at, cols] = value.astype(jnp.bfloat16)

    @pl.loop(0, SUBS + n - 1)
    def _(wave):
        @pl.when(wave + AHEAD < SUBS)
        def _():
            for d in range(2):
                hop(1, wave + AHEAD, d, mine(wave + AHEAD, d)).start()

        for s in range(1, n):
            i = wave - (s - 1)

            @pl.when((i >= 0) & (i < SUBS))
            def _():
                for d in range(2):
                    hop(s, i, d, piece(s, i, d, core)).wait_recv()
                    if s < n - 1:
                        hop(s + 1, i, d, piece(s, i, d, core)).start()
                    push(s, i, d, piece(s, i, d, core)).start()

            if s == 1:

                @pl.when(wave < SUBS)
                def _():
                    for d in range(2):
                        keep(wave, d).wait()
                    multiply(0, wave)

            @pl.when((i >= 1) & (i <= SUBS))
            def _():
                multiply(s, i - 1)
                if s == n - 1:
                    activate(i - 1)

    @pl.loop(0, SUBS)
    def _(i):
        for d in range(2):
            for s in range(n):
                push(s, i, d, piece(s, i, d, core)).wait_send()
            for s in range(1, n):
                hop(s, i, d, piece(s, i, d, core)).wait_send()


def gather_matmul(n, feats, gains, perturbed):
    tokens, depth = feats.shape
    rows, cols = perturbed.shape
    half = cols // 2
    dma = pltpu.SemaphoreType.DMA
    return pl.pallas_call(
        functools.partial(gather_kernel, n),
        out_shape=jax.ShapeDtypeStruct((tokens, cols), jnp.bfloat16),
        in_specs=[
            pl.BlockSpec(memory_space=pl.ANY),
            pl.BlockSpec(memory_space=pltpu.VMEM),
            pl.BlockSpec(memory_space=pl.ANY),
        ],
        out_specs=pl.BlockSpec(memory_space=pltpu.VMEM),
        scratch_shapes=[
            pltpu.VMEM((tokens, depth), jnp.bfloat16),
            pltpu.VMEM((n, 2, SUBS, 2 * rows, half // SUBS), jnp.bfloat16),
            pltpu.VMEM((tokens, cols), jnp.float32),
            dma(((n - 1) * SUBS * 2,)),
            dma(((n - 1) * SUBS * 2,)),
            dma((n * SUBS * 2,)),
            dma((n * SUBS * 2,)),
            dma((SUBS * 2,)),
            dma((1,)),
        ],
        compiler_params=pltpu.CompilerParams(
            collective_id=2, has_side_effects=True, vmem_limit_bytes=VMEM_LIMIT
        ),
        cost_estimate=pl.CostEstimate(
            flops=2 * tokens * depth * cols,
            bytes_accessed=2 * depth * cols,
            transcendentals=0,
        ),
        name="gather_matmul",
    )(feats, gains, perturbed)


def ring_program(n, n_mp, radius, tokens, ln_gain, weights, grad_partials):
    feats = lax.all_gather(tokens, "mp", axis=1, tiled=True)
    gain = jnp.broadcast_to(ln_gain.astype(jnp.float32), (8, ln_gain.shape[0]))
    perturbed, gains = reduce_rows(n, n_mp, radius, grad_partials[0], weights, gain)
    hidden = gather_matmul(n, feats, gains[:, 0].reshape(1, -1), perturbed)
    return (hidden, perturbed)


def grid_kernel(
    n_mp, radius, x_ref, gain_ref, g_ref, w_ref, hid, wnew,
    part0, part1, recv0, recv1, own0, own1, grad, sq0, sq1, near, far,
    turned, zstat, stat, lead, landed,
    push_send, push_recv, hop_send, hop_recv, own_sem, load_sem,
    z_send, z_recv, stat_send, stat_recv,
    cross_send, cross_recv, relay_send, relay_recv, spread_send, spread_recv,
    y_send, y_recv, mine_send, mine_recv, pass_send, pass_recv, c_send, c_recv,
    head_send, head_recv,
):
    part, recv, own, sq = (part0, part1), (recv0, recv1), (own0, own1), (sq0, sq1)
    me, z = lax.axis_index("dp"), lax.axis_index("mp")
    core, x, y = me % 2, (me // 2) % 2, me // 4
    rows, width = part0.shape[1], (part0.shape[2], part1.shape[2])
    start_col = (0, width[0])
    sub, tile, tokens, feats = rows // SUBS, 16, hid.shape[0], near.shape[2]
    chunks = (width[0] // CHUNK, width[1] // CHUNK)

    def device(flip_x, flip_y, which):
        cx = 1 - x if flip_x else x
        cy = 1 - y if flip_y else y
        return (cy * 2 + cx) * 2 + which

    partner, x_peer, y_peer = device(0, 0, 1 - core), device(1, 0, core), device(0, 1, core)
    flips = (((1, 1), (1, 0), (0, 1), (0, 0)), ((1, 1), (0, 1), (1, 0), (0, 0)))
    hops = ((x_peer, x_peer, y_peer), (y_peer, y_peer, x_peer))
    everyone = [
        {"dp": (me + a) % 8, "mp": (z + b) % n_mp} for a in range(8) for b in range(n_mp) if a + b
    ]

    mine, ours = 2 * y + core, 2 * y + 1 - core
    theirs, others_there = 2 * (1 - y) + core, 2 * (1 - y) + 1 - core

    def span(i, size):
        return pl.ds(pl.multiple_of(i * size, size), size)

    def block(s, i, d, which):
        start = device(*flips[d][s], which) * rows + i * sub
        return g_ref.at[pl.ds(pl.multiple_of(start, tile), sub), pl.ds(start_col[d], width[d])]

    def piece(ref, s, i):
        return ref.at[s, span(i, sub)]

    def push(s, i, d):
        at = (s * SUBS + i) * 2 + d
        return remote(
            block(s, i, d, 1 - core), piece(part[d], s, i), push_send.at[d], push_recv.at[at], partner
        )

    def load(s, i, d, slot):
        return pltpu.make_async_copy(block(s, i, d, core), own[d].at[slot], own_sem.at[slot * 2 + d])

    def hop(s, i, d):
        at = (s * SUBS + i) * 2 + d
        return remote(
            piece(part[d], s, i), piece(recv[d], s, i), hop_send.at[d], hop_recv.at[at], hops[d][s]
        )

    def add(s, i, slot):
        for d in range(2):
            load(s, i, d, slot).wait()
            push(s, i, d).wait_recv()
            came = {0: (), 1: (), 2: (0,), 3: (1, 2)}[s]
            if s > 1:
                hop(2 * s - 4, i, d).wait_recv()
            source, mine = piece(part[d], s, i), own[d].at[slot]
            extra = [piece(recv[d], k, i) for k in came]

            @pl.loop(0, sub // tile)
            def _(r):
                at = span(r, tile)
                value = mine[at, :].astype(jnp.float32) + source[at, :].astype(jnp.float32)
                for ref in extra:
                    value = value + ref[at, :].astype(jnp.float32)
                if s == 3:
                    row = pl.multiple_of(i * sub + r * tile, tile)
                    grad[pl.ds(row, tile), start_col[d] : start_col[d] + width[d]] = value
                    squared = value * value
                    sq[d][...] += squared[:8] + squared[8:]
                else:
                    source[at, :] = value.astype(jnp.bfloat16)

            if s < 3:
                hop(s, i, d).start()

    def both(make, *args):
        for d in range(2):
            make(*args[:2], d, *args[2:]).start()

    fetch = pltpu.make_async_copy(x_ref, hid.at[:, pl.ds(0, feats)], load_sem.at[0])
    fetch_w = pltpu.make_async_copy(w_ref, wnew, load_sem.at[1])
    tall, lines = turned.shape[1], 64

    def z_copy(k):
        return remote(
            zstat.at[z], zstat.at[z], z_send.at[k], z_recv.at[k], (z + k + 1) % n_mp, "mp"
        )

    def gather_statistics():
        fetch.wait()

        @pl.loop(0, tokens // tall)
        def _(b):
            @pl.loop(0, tall // lines)
            def _(r):
                at = pl.ds(pl.multiple_of(b * tall + r * lines, lines), lines)
                values = hid[at, :feats].astype(jnp.float32)
                center = jnp.mean(values, axis=1, keepdims=True)
                moved = values - center
                spread = jnp.sum(moved * moved, axis=1, keepdims=True)
                turned[0, span(r, lines), :] = jnp.broadcast_to(center, (lines, tall))
                turned[1, span(r, lines), :] = jnp.broadcast_to(spread, (lines, tall))

            for k in range(2):
                zstat[z, k, b] = turned[k].T[:8]

        for k in range(n_mp - 1):
            z_copy(k).start()

    belongs = (z + x) % 2 == 0
    half = tokens // 2

    def cross_copy(send):
        src = hid.at[pl.ds(0, half), pl.ds(0, feats)] if send == 0 else relay_room
        return remote(
            src, far.at[z // 2, pl.ds(send * half, half)], cross_send.at[0], cross_recv.at[0], x_peer
        )

    relay_room = hid.at[pl.ds(0, half), pl.ds(feats, feats)]
    relay_copy = remote(
        hid.at[pl.ds(half, half), pl.ds(0, feats)], relay_room,
        relay_send.at[0], relay_recv.at[0], z + 1 - 2 * (z % 2), "mp",
    )

    ends = ((3 * x, x), (2 - x, 1 - x))
    items = [(o, near.at[k, pl.ds(h * half, half)]) for o, k in ends for h in range(2)]
    items += [(x + 2 * k, far.at[k, pl.ds(0, half)]) for k in range(2)]
    items += [(1 - x + 2 * k, far.at[k, pl.ds(half, half)]) for k in range(2)]
    near_top, long_low, short_low, far_top, far_low = (0, 2), (1,), (3,), (4, 5), (6, 7)

    def spread_copy(k, way):
        return remote(
            items[k][1], items[k][1], spread_send.at[k * 2 + way], spread_recv.at[k],
            z + 1 - 2 * way, "mp",
        )

    def spread(which, steps):
        for k in which:
            away = z - items[k][0]
            if steps == 0 and k >= 4:

                @pl.when(away == 0)
                def _():
                    cross_copy(0).wait_recv()

            for way, sign in ((0, 1), (1, -1)):
                @pl.when((away * sign == steps) & ((z < n_mp - 1) if way == 0 else (z > 0)))
                def _():
                    if steps > 0:
                        spread_copy(k, way).wait_recv()
                    spread_copy(k, way).start()

    def spread_arrived(which):
        for k in which:
            away = z - items[k][0]

            @pl.when(((z == 0) & (away < 0)) | ((z == n_mp - 1) & (away > 0)))
            def _():
                spread_copy(k, 0).wait_recv()

    def spread_sent():
        for k in range(8):
            away = z - items[k][0]

            @pl.when((away >= 0) & (z < n_mp - 1))
            def _():
                spread_copy(k, 0).wait_send()

            @pl.when((away <= 0) & (z > 0))
            def _():
                spread_copy(k, 1).wait_send()

        cross_copy(0).wait_send()

        @pl.when((z + x) % 2 == 1)
        def _():
            relay_copy.wait_send()

    def normalise():
        for k in range(n_mp - 1):
            z_copy(k).wait_recv()
        centers = [zstat[k, 0] for k in range(n_mp)]
        center = sum(centers) * (1.0 / n_mp)
        squared = sum(zstat[k, 1] for k in range(n_mp))
        squared = squared + feats * sum((one - center) * (one - center) for one in centers)
        scaled = 1.0 / jnp.sqrt(squared * (1.0 / (feats * n_mp)) + 1e-06)
        for k in range(n_mp - 1):
            z_copy(k).wait_send()
        zstat[0, 0] = center
        zstat[0, 1] = scaled

        for h in range(2):
            @pl.loop(h * half // tall, (h + 1) * half // tall)
            def _(b):
                for k in range(2):
                    turned[k] = jnp.broadcast_to(zstat[0, k, b][:1], (tall, tall)).T

                @pl.loop(0, tall // lines)
                def _(r):
                    at = pl.ds(pl.multiple_of(b * tall + r * lines, lines), lines)
                    values = hid[at, :feats].astype(jnp.float32)
                    moved = values - turned[0, span(r, lines), :1]
                    value = moved * turned[1, span(r, lines), :1] * gain_ref[...].astype(jnp.float32).reshape(1, feats)
                    value = value.astype(jnp.bfloat16)
                    hid[at, :feats] = value

                    @pl.when(belongs)
                    def _():
                        near[z // 2, at, :] = value

            @pl.when((z + x) % 2 == 1)
            def _():
                (cross_copy(0) if h == 0 else relay_copy).start()

            spread(near_top if h == 0 else long_low + short_low, 0)

    def relay():
        @pl.when(belongs)
        def _():
            relay_copy.wait_recv()
            cross_copy(1).start()

    def events(i, table):
        for k, actions in table.items():
            @pl.when(i == k)
            def _():
                for action in actions:
                    action()

    def later(which, steps):
        return lambda: spread(which, steps)

    fetch.start()
    both(load, 0, 0, 0)
    sq0[...] = jnp.zeros_like(sq0)
    sq1[...] = jnp.zeros_like(sq1)
    greet(everyone)

    @pl.loop(0, SUBS)
    def _(i):
        both(push, 0, i)

    @pl.loop(0, SUBS)
    def _(i):
        @pl.when(i + 1 < SUBS)
        def _():
            both(load, 0, i + 1, (i + 1) % 2)

        @pl.when(i + 1 == SUBS)
        def _():
            both(load, 1, 0, 0)

        both(push, 1, i)
        both(push, 2, i)
        add(0, i, i % 2)
        events(i, {0: [gather_statistics], 2: [normalise]})

    @pl.loop(0, SUBS)
    def _(i):
        both(load, 2, i, 1)
        both(push, 3, i)
        add(1, i, 0)

        @pl.when(i + 1 < SUBS)
        def _():
            both(load, 1, i + 1, 0)

        @pl.when(i + 1 == SUBS)
        def _():
            both(load, 3, 0, 0)

        add(2, i, 1)
        events(
            i,
            {
                0: [relay],
                2: [later(near_top, 1)],
                3: [later(far_top, 0)],
                4: [later(short_low, 1)],
            },
        )

    fetch_w.start()

    @pl.loop(0, SUBS)
    def _(i):
        @pl.when(i + 1 < SUBS)
        def _():
            both(load, 3, i + 1, (i + 1) % 2)

        for d in range(2):
            hop(1, i, d).wait_recv()
        events(
            i,
            {
                0: [later(near_top, 2), later(far_low, 0)],
                3: [later(far_top, 2), later(far_low, 2)],
            },
        )
        add(3, i, i % 2)
        events(i, {0: [later(far_top, 1)], 1: [later(far_low, 1)], 2: [later(long_low, 1)]})

    folded = jnp.zeros((8, 128), jnp.float32)
    for d in range(2):
        for c in range(width[d] // 128):
            folded = folded + sq[d][:, c * 128 : (c + 1) * 128]
    stat[0] = folded

    for d in range(2):
        remote(part[d], part[d], push_send.at[d], push_recv.at[0], partner).wait_send()
        sent = part[d].at[pl.ds(0, 3)]
        remote(sent, recv[d], hop_send.at[d], hop_recv.at[0], partner).wait_send()

    def shared(src, dst, device_id):
        return pltpu.make_async_remote_copy(
            src_ref=src,
            dst_ref=dst,
            send_sem=stat_send.at[0],
            recv_sem=stat_recv.at[0],
            device_id=device_id,
            device_id_type=pl.DeviceIdType.MESH,
        )

    for k, device_id in enumerate(everyone):
        shared(stat.at[pl.ds(0, 1)], stat.at[pl.ds(k + 1, 1)], device_id).start()
    fetch_w.wait()

    top = rows // 2

    def head(k):
        here = part0.at[mine, pl.ds(top, top), pl.ds(0, CHUNK)]
        src = (wnew.at[pl.ds(0, top), pl.ds(0, CHUNK)], lead, here)[k]
        dst = (landed.at[0], landed.at[1], here)[k]
        return remote(src, dst, head_send.at[k], head_recv.at[k], y_peer)

    head(0).start()
    lead[...] = grad[:top, :CHUNK].astype(jnp.bfloat16)
    head(1).start()
    rest = stat.at[pl.ds(1, len(everyone))]
    shared(rest, rest, everyone[0]).wait()
    every = jnp.sum(stat[...], axis=0)
    squares = jnp.sum(jnp.sum(every, axis=0, keepdims=True), axis=1, keepdims=True)
    scale = radius / jnp.sqrt(squares + 1e-12)


    def slab(d, slot, j):
        return part[d].at[slot, :, span(j, CHUNK)]

    def across(d, j):
        at = d * chunks[0] + j
        here = slab(d, mine, j)
        return remote(here, here, y_send.at[d], y_recv.at[at], y_peer)

    def across_arrived(d, j):
        at = d * chunks[0] + j
        here = slab(d, theirs, j)
        return remote(here, here, y_send.at[d], y_recv.at[at], y_peer)

    def give(d, j, slot):
        at = d * chunks[0] + j
        here = slab(d, mine if slot == "mine" else theirs, j)
        sems = (mine_send, mine_recv) if slot == "mine" else (pass_send, pass_recv)
        return remote(here, here, sems[0].at[d], sems[1].at[at], partner)

    def given(d, j, slot):
        at = d * chunks[0] + j
        here = slab(d, ours if slot == "mine" else others_there, j)
        sems = (mine_send, mine_recv) if slot == "mine" else (pass_send, pass_recv)
        return remote(here, here, sems[0].at[d], sems[1].at[at], partner)

    def partial_copy(d, j):
        at = d * chunks[0] + j
        return remote(
            recv[d].at[0, :, span(j, CHUNK)], recv[d].at[1, :, span(j, CHUNK)],
            c_send.at[d], c_recv.at[at], x_peer,
        )

    def columns(d, j):
        return pl.ds(pl.multiple_of(start_col[d] + j * CHUNK, 128), CHUNK)

    def perturb(d, j):
        cols = columns(d, j)

        @pl.loop(0, rows // 256)
        def _(r):
            at = span(r, 256)
            value = wnew[at, cols].astype(jnp.float32) + scale * grad[at, cols]
            value = value.astype(jnp.bfloat16)
            wnew[at, cols] = value
            part[d][mine, at, span(j, CHUNK)] = value

    for k in range(2):
        head(k).wait_send()
    perturb(0, 0)
    head(2).start()
    give(0, 0, "mine").start()
    for d in range(2):
        @pl.loop(1 - d, chunks[d])
        def _(j):
            perturb(d, j)
            across(d, j).start()

    def give_next(d, j):
        @pl.when(j + 1 < chunks[d])
        def _():
            give(d, j + 1, "mine").start()

        if d == 0:

            @pl.when(j + 1 == chunks[0])
            def _():
                give(1, 0, "mine").start()

    def arrive_first():
        for k in range(2):
            head(k).wait_recv()
        value = landed[0].astype(jnp.float32) + scale * landed[1].astype(jnp.float32)
        part0[theirs, :top, :CHUNK] = value.astype(jnp.bfloat16)
        there = part0.at[theirs, pl.ds(top, top), pl.ds(0, CHUNK)]
        remote(there, there, head_send.at[2], head_recv.at[2], y_peer).wait_recv()
        give(0, 0, "theirs").start()
        give_next(0, 0)

    def product(left, at, d, j, size):
        total = None
        for k in range(2):
            right = part[d][2 * k : 2 * k + 2, :, span(j, size)].reshape(2 * rows, size)
            one = jnp.dot(left[k, at], right, preferred_element_type=jnp.float32)
            total = one if total is None else total + one
        return total

    def arrive(d, j):
        across_arrived(d, j).wait_recv()
        give(d, j, "theirs").start()
        give_next(d, j)

    def send_far(d, j):
        given(d, j, "mine").wait_recv()
        given(d, j, "theirs").wait_recv()
        recv[d][0, :, span(j, CHUNK)] = product(far, pl.ds(0, tokens), d, j, CHUNK).astype(jnp.bfloat16)
        partial_copy(d, j).start()

    def keep_near(d, g, h):
        size, at = GROUP * CHUNK, pl.ds(h * half, half)
        cols = pl.ds(pl.multiple_of(start_col[d] + g * size, 128), size)
        grad[at, cols] = product(near, at, d, g, size)

    def settle(d):
        here, there, partial = part[d].at[mine], part[d].at[theirs], recv[d].at[0]
        first = CHUNK * (1 - d)
        sent = part[d].at[mine, :, pl.ds(first, width[d] - first)]
        remote(sent, sent, y_send.at[d], y_recv.at[0], y_peer).wait_send()
        remote(here, here, mine_send.at[d], mine_recv.at[0], partner).wait_send()
        remote(there, there, pass_send.at[d], pass_recv.at[0], partner).wait_send()
        remote(partial, partial, c_send.at[d], c_recv.at[0], x_peer).wait_send()

    def finish(d, j):
        cols = columns(d, j)
        partial_copy(d, j).wait_recv()

        @pl.loop(0, tokens // 64)
        def _(r):
            at = span(r, 64)
            pre = grad[at, cols] + recv[d][1, at, span(j, CHUNK)].astype(jnp.float32)
            value = 0.5 * pre * (1.0 + lax.erf(pre * math.sqrt(0.5)))
            hid[at, cols] = value.astype(jnp.bfloat16)

    spread(long_low, 2)
    spread_arrived(far_top + far_low)

    arrive_first()
    send_far(0, 0)

    @pl.loop(1, chunks[0])
    def _(j):
        arrive(0, j)
        send_far(0, j)

    spread_arrived(near_top + long_low + short_low)
    groups = (chunks[0] // GROUP, chunks[1] // GROUP)
    turns = [0, 1] + [2 + GROUP * k for k in range(2 * groups[0] - 2)]
    spread_sent()

    @pl.loop(0, chunks[1])
    def _(j):
        arrive(1, j)

        @pl.when((j % GROUP == 0) & (j > 0))
        def _():
            keep_near(1, j // GROUP - 1, 0)

        @pl.when((j % GROUP == 1) & (j > 1))
        def _():
            keep_near(1, j // GROUP - 1, 1)

        for k, turn in enumerate(turns):
            @pl.when(j == turn)
            def _():
                keep_near(0, k // 2, k % 2)

        send_far(1, j)

        @pl.when(j >= GROUP + 2)
        def _():
            finish(1, j - GROUP - 2)

        for g in range(groups[0]):
            for k in range(GROUP):
                @pl.when(j == turns[2 * g + 1] + 1 + k)
                def _():
                    finish(0, g * GROUP + k)

    for h in range(2):
        keep_near(1, groups[1] - 1, h)
    for j in range(max(chunks[1] - turns[-1] - 1, 0), GROUP):
        finish(0, chunks[0] - GROUP + j)
    for j in range(chunks[1] - GROUP - 2, chunks[1]):
        finish(1, j)

    head(2).wait_send()
    for d in range(2):
        settle(d)


def store_kernel(hid, weights, hid_out, w_out, sem):
    strip = hid.shape[0] // STRIPS
    copies = []
    for k, (src, dst) in enumerate(((hid, hid_out), (weights, w_out))):
        for i in range(STRIPS):
            at = pl.ds(i * strip, strip)
            copies.append(pltpu.make_async_copy(src.at[at], dst.at[at], sem.at[k * STRIPS + i]))
    for copy in copies:
        copy.start()
    for copy in copies:
        copy.wait()


def store(hid, weights):
    anywhere, inside = pl.BlockSpec(memory_space=pl.ANY), pl.BlockSpec(memory_space=pltpu.VMEM)
    hid = pltpu.with_memory_space_constraint(hid, pltpu.VMEM)
    weights = pltpu.with_memory_space_constraint(weights, pltpu.VMEM)
    return pl.pallas_call(
        store_kernel,
        out_shape=(
            jax.ShapeDtypeStruct(hid.shape, hid.dtype),
            jax.ShapeDtypeStruct(weights.shape, weights.dtype),
        ),
        in_specs=[inside, inside],
        out_specs=(anywhere, anywhere),
        scratch_shapes=[pltpu.SemaphoreType.DMA((2 * STRIPS,))],
        compiler_params=pltpu.CompilerParams(vmem_limit_bytes=1000000),
        name="store",
    )(hid, weights)


def grid_program(n_mp, radius, tokens, gain, weights, grads):
    depth, cols = grads.shape
    rows = depth // 8
    count, feats = tokens.shape
    unit = GROUP * CHUNK
    first = cols * 3 // 8 // unit * unit
    wide = (first, cols - first)
    sub, pieces = rows // SUBS, cols // CHUNK
    dma = pltpu.SemaphoreType.DMA
    bf16, f32 = jnp.bfloat16, jnp.float32
    anywhere = pl.BlockSpec(memory_space=pl.ANY)
    return pl.pallas_call(
        functools.partial(grid_kernel, n_mp, radius),
        out_shape=(
            pltpu.VMEM((count, cols), bf16),
            pltpu.VMEM((rows, cols), bf16),
        ),
        in_specs=[anywhere, pl.BlockSpec(memory_space=pltpu.VMEM), anywhere, anywhere],
        out_specs=(pl.BlockSpec(memory_space=pltpu.VMEM), pl.BlockSpec(memory_space=pltpu.VMEM)),
        scratch_shapes=[
            pltpu.VMEM((4, rows, wide[0]), bf16),
            pltpu.VMEM((4, rows, wide[1]), bf16),
            pltpu.VMEM((3, rows, wide[0]), bf16),
            pltpu.VMEM((3, rows, wide[1]), bf16),
            pltpu.VMEM((2, sub, wide[0]), bf16),
            pltpu.VMEM((2, sub, wide[1]), bf16),
            pltpu.VMEM((rows, cols), f32),
            pltpu.VMEM((8, wide[0]), f32),
            pltpu.VMEM((8, wide[1]), f32),
            pltpu.VMEM((2, count, feats), bf16),
            pltpu.VMEM((2, count, feats), bf16),
            pltpu.VMEM((2, 128, 128), f32),
            pltpu.VMEM((n_mp, 2, count // 128, 8, 128), f32),
            pltpu.VMEM((8 * n_mp, 8, 128), f32),
            pltpu.VMEM((rows // 2, CHUNK), bf16),
            pltpu.VMEM((2, rows // 2, CHUNK), bf16),
            dma((2,)),
            dma((8 * SUBS,)),
            dma((2,)),
            dma((6 * SUBS,)),
            dma((4,)),
            dma((2,)),
            dma((n_mp - 1,)),
            dma((n_mp - 1,)),
            dma((1,)),
            dma((1,)),
            dma((1,)),
            dma((1,)),
            dma((1,)),
            dma((1,)),
            dma((16,)),
            dma((8,)),
        ]
        + [dma((2,)), dma((pieces,))] * 4
        + [dma((3,))] * 2,
        compiler_params=pltpu.CompilerParams(
            collective_id=3, has_side_effects=True, vmem_limit_bytes=57000000
        ),
        name="grid_program",
    )(tokens, gain, grads, weights)


def per_device(n, n_mp, width, tokens, ln_gain, weights, grad_partials):
    radius = 0.7 * math.sqrt(width)
    if n == 4 and n_mp == 4 and weights.shape[1] % (8 * GROUP * CHUNK) == 0:
        return store(*grid_program(n_mp, radius, tokens, ln_gain, weights, grad_partials[0]))
    return ring_program(n, n_mp, radius, tokens, ln_gain, weights, grad_partials)


def solution(mesh):
    placed = (P("dp", "mp"), P("mp"), P("dp", "mp"), P("dp", None, "mp"))

    def whole(tokens, ln_gain, weights, grad_partials):
        return jax.shard_map(
            functools.partial(per_device, mesh.shape["dp"] // 2, mesh.shape["mp"], weights.shape[1]),
            mesh=mesh,
            in_specs=placed,
            out_specs=(P("dp", "mp"), P("dp", "mp")),
            check_vma=False,
        )(tokens, ln_gain, weights, grad_partials)

    return whole
```
